512 devices in a mesh: gx: 8 (over y_lo, x), gy: 8 (over z), gz: 8 (over y_hi, core).
Axes of the slice: x: 4, y: 8 (y_hi: 4, y_lo: 2; y = y_hi * 2 + y_lo), z: 8, core: 2. Of those that a mesh axis runs over, the one named last changes fastest.
Arguments:
- material: int32 [256, 512, 1024], P('gx', 'gy', 'gz'), may hold values from 0 to 7
- eps_table: float32 [8], replicated, may hold values from 1 to 13
- grading: bfloat16 [256, 512, 1024], P('gx', 'gy', 'gz'), may hold values from 0.25 to 1.75
Outputs:
- smoothed: bfloat16 [6, 256, 512, 1024], P(None, 'gx', 'gy', 'gz')
The draws below stay inside these ranges and needn't reach their ends.
All inputs are finite; a program needn't handle non-finite values.
Results may differ from the reference program's by a relative error of at most 0.001.
Values sent between devices are 32-bit elements; how exact they have to be, the bound alone decides.
No kernel may reach another device: no remote copies, remote signals or barrier semaphores. Data moves between devices by JAX's collectives and lax.ppermute only.
A program may use at most 64 MiB of HBM per device.

```python
import math
import jax
import jax.numpy as jnp

MATERIALS = 8
NX = 256
NY = 512
NZ = 1024


def touch_ends(drawn, rng, low, top_value):
    dims = drawn.shape
    spot = [jax.random.randint(jax.random.fold_in(rng, axis), (), 0, dims[axis]) for axis in range(len(dims))]
    drawn = drawn.at[tuple(spot)].set(low)
    longest = dims.index(max(dims))
    spot[longest] = (spot[longest] + 1) % dims[longest]
    return drawn.at[tuple(spot)].set(top_value)


def setup_inputs(seed: int = 0) -> dict:
    seeds = jax.random.split(jax.random.key(seed), 4)
    return {
        "material": touch_ends(jax.random.randint(seeds[0], (NX, NY, NZ), 0, MATERIALS), jax.random.fold_in(seeds[0], 1), 0, MATERIALS - 1).astype(jnp.int32),
        "eps_table": jnp.clip(jnp.exp(jax.random.uniform(seeds[1], (MATERIALS,), jnp.float32, math.log(1.0), math.log(13.0))), 1.0, 13.0),
        "grading": jnp.clip(1.0 + 0.15 * jax.random.normal(seeds[2], (NX, NY, NZ), jnp.float32), 0.25, 1.75).astype(jnp.bfloat16),
    }


def lookup(material, eps_table, grading):
    values = jnp.zeros(material.shape, jnp.float32)
    for index in range(eps_table.shape[0]):
        values = jnp.where(material == index, eps_table[index], values)
    return values * grading.astype(jnp.float32)


def box_mean(padded):
    total = padded[:-2] + padded[1:-1] + padded[2:]
    total = total[:, :-2] + total[:, 1:-1] + total[:, 2:]
    total = total[:, :, :-2] + total[:, :, 1:-1] + total[:, :, 2:]
    return total / 27.0


def tensor(mean_ext, mean_inv):
    centre = mean_ext[1:-1, 1:-1, 1:-1]
    grad_x = (mean_ext[2:, 1:-1, 1:-1] - mean_ext[:-2, 1:-1, 1:-1]) * 0.5
    grad_y = (mean_ext[1:-1, 2:, 1:-1] - mean_ext[1:-1, :-2, 1:-1]) * 0.5
    grad_z = (mean_ext[1:-1, 1:-1, 2:] - mean_ext[1:-1, 1:-1, :-2]) * 0.5
    scale = 1.0 / (grad_x * grad_x + grad_y * grad_y + grad_z * grad_z + 0.1)
    recip = 1.0 / centre
    grads = (grad_x, grad_y, grad_z)
    pairs = ((0, 0), (1, 1), (2, 2), (0, 1), (0, 2), (1, 2))
    result = []
    for first, second in pairs:
        weight = grads[first] * grads[second] * scale
        delta = 1.0 if first == second else 0.0
        result.append(mean_inv * weight + (delta - weight) * recip)
    return jnp.stack(result, 0).astype(jnp.bfloat16)


def reference(material, eps_table, grading):
    eps = lookup(material, eps_table, grading)
    padded = jnp.pad(eps, 2, mode="wrap")
    mean_ext = box_mean(padded)
    mean_inv = box_mean(1.0 / padded)[1:-1, 1:-1, 1:-1]
    return tensor(mean_ext, mean_inv)
```

```python
import jax
import jax.numpy as jnp
from jax import lax
from jax.experimental import pallas as pl
from jax.experimental.pallas import tpu as pltpu
from jax.sharding import PartitionSpec as P

F32 = jnp.float32
VMEM = pl.BlockSpec(memory_space=pltpu.VMEM)
SMEM = pl.BlockSpec(memory_space=pltpu.SMEM)
ANY = pl.BlockSpec(memory_space=pl.ANY)


def lookup(material, table, grading):
    low = (material & 1) != 0
    mid = (material & 2) != 0
    top = (material & 4) != 0
    pair = [jnp.where(low, table[2 * k + 1], table[2 * k]) for k in range(4)]
    quad = [jnp.where(mid, pair[2 * k + 1], pair[2 * k]) for k in range(2)]
    return jnp.where(top, quad[1], quad[0]) * grading.astype(F32)


def lanes(shape):
    return lax.broadcasted_iota(jnp.int32, shape, len(shape) - 1)


def scalars(table_ref):
    return [table_ref[k] for k in range(8)]


def faces_kernel(table_ref, mat_low, mat_high, gra_low, gra_high, fwd_ref, bwd_ref):
    table = scalars(table_ref)
    nx = mat_low.shape[0]
    lane = lanes((8, 128))
    packed = [jnp.zeros((8, 128), F32)] * 2
    for x in range(nx):
        low = lookup(mat_low[x], table, gra_low[x, 0:8])
        high = lookup(mat_high[x], table, gra_high[x, 8:16])
        bwd_ref[2 * x : 2 * x + 2] = low[0:2]
        fwd_ref[2 * x : 2 * x + 2] = high[6:8]
        here = (lane >> 2) == x
        turn = (4 * x + 2) % 128
        packed = [
            jnp.where(here, pltpu.roll(v, turn, 1) if turn else v, p)
            for v, p in zip((low, high), packed)
        ]
    ones = jnp.ones((6, 128), F32)
    for ref, rows in ((bwd_ref, packed[0][0:2]), (fwd_ref, packed[1][6:8])):
        ref[2 * nx : 2 * nx + 2] = rows
        ref[2 * nx + 2 : 2 * nx + 8] = ones


def block_kernel(table_ref, mat_ref, gra_ref, eps_ref, packed_ref):
    table = scalars(table_ref)
    step = mat_ref.shape[0]
    first = pl.program_id(0) * step
    lane = lanes(mat_ref.shape[1:])

    @pl.when(first == 0)
    def _():
        packed_ref[...] = jnp.zeros(packed_ref.shape, F32)

    packed = packed_ref[...]
    for k in range(step):
        value = lookup(mat_ref[k], table, gra_ref[k])
        eps_ref[k] = value
        x = first + k
        packed = jnp.where(
            (lane >> 2) == x, pltpu.roll(value, lax.rem(4 * x + 2, 128), 1), packed
        )
    packed_ref[...] = packed


def zface_kernel(packed_ref, low_ref, high_ref, out_ref):
    ny = packed_ref.shape[0]
    out_ref[0:ny] = packed_ref[...]
    out_ref[ny : ny + 2] = low_ref[64:66]
    out_ref[ny + 2 : ny + 4] = high_ref[64:66]
    out_ref[ny + 4 : ny + 8] = jnp.ones((4, 128), F32)


def joined(parity_ref, even_ref, odd_ref):
    lane = lanes(even_ref.shape)
    return jnp.where(((lane >> 1) & 1) == parity_ref[0], odd_ref[...], even_ref[...])


def xface_kernel(parity_ref, eps_ref, low_ref, high_ref, even_ref, odd_ref, fwd_ref, bwd_ref):
    nx, ny = eps_ref.shape[0], eps_ref.shape[1]
    rows = ny + 8
    halo = joined(parity_ref, even_ref, odd_ref)
    lane = lanes((8, 128))
    for ref, start in ((fwd_ref, nx - 2), (bwd_ref, 0)):
        for s in range(2):
            x = start + s
            ref[s * rows : s * rows + ny] = eps_ref[x]
            ref[s * rows + ny : s * rows + ny + 2] = low_ref[2 * x : 2 * x + 2]
            ref[s * rows + ny + 2 : s * rows + ny + 4] = high_ref[2 * x : 2 * x + 2]
            ref[s * rows + ny + 4 : s * rows + rows] = jnp.ones((4, 128), F32)
        packed = jnp.ones((8, 128), F32)
        for g in range(rows // 8):
            turn = (8 * g - 4 * start) % 128
            part = halo[8 * g : 8 * g + 8]
            packed = jnp.where((lane >> 3) == g, pltpu.roll(part, turn, 1) if turn else part, packed)
        ref[2 * rows : 2 * rows + 8] = packed


def zsums(v, h, lane):
    left = pltpu.roll(jnp.where(lane == 127, h, v), 1, 1)
    left2 = pltpu.roll(jnp.where(lane >= 126, h, v), 2, 1)
    right = pltpu.roll(jnp.where(lane == 0, h, v), 127, 1)
    right2 = pltpu.roll(jnp.where(lane <= 1, h, v), 126, 1)
    inv, inv_h = 1.0 / v, 1.0 / h
    inv_left = pltpu.roll(jnp.where(lane == 127, inv_h, inv), 1, 1)
    inv_right = pltpu.roll(jnp.where(lane == 0, inv_h, inv), 127, 1)
    return v + left + right, (right + right2) - (left + left2), inv + inv_left + inv_right


def put(ref, index, value, ny):
    ref[index, 8 : 8 + ny] = value[0:ny]
    ref[index, 6:8] = value[ny : ny + 2]
    ref[index, 8 + ny : 10 + ny] = value[ny + 2 : ny + 4]


def ysums(refs, index, ny):
    box, der, inv = refs
    b = [box[index, 8 + k : 8 + k + ny] for k in (-2, -1, 0, 1, 2)]
    d = [der[index, 8 + k : 8 + k + ny] for k in (-1, 0, 1)]
    i = [inv[index, 8 + k : 8 + k + ny] for k in (-1, 0, 1)]
    return (
        b[1] + b[2] + b[3],
        (b[4] + b[3]) - (b[1] + b[0]),
        d[0] + d[1] + d[2],
        i[0] + i[1] + i[2],
    )


def result(yb, yd, zd, yi):
    mean = yb[1] + yb[2] + yb[3]
    gx = (yb[4] + yb[3]) - (yb[1] + yb[0])
    gy = yd[0] + yd[1] + yd[2]
    gz = zd[0] + zd[1] + zd[2]
    inv = yi[0] + yi[1] + yi[2]
    recip = 27.0 / mean
    factor = (inv * (1.0 / 27.0) - recip) / (gx * gx + gy * gy + gz * gz + 291.6)
    fx, fy, fz = gx * factor, gy * factor, gz * factor
    return (gx * fx + recip, gy * fy + recip, gz * fz + recip, gx * fy, gx * fz, gy * fz)


CHUNK = 4


def inner_kernel(
    parity_ref, eps_ref, low_ref, high_ref, even_ref, odd_ref,
    out_ref, yb_out, yd_out, zd_out, yi_out,
    rim, halo, box, der, inv, yb, yd, zd, yi, obuf, sem,
):
    nx, ny = eps_ref.shape[0], eps_ref.shape[1]
    halo[...] = joined(parity_ref, even_ref, odd_ref)
    lane = lanes((ny + 8, 128))
    ones = jnp.ones((4, 128), F32)
    for x in range(nx):
        rim[x, 0:2] = low_ref[2 * x : 2 * x + 2]
        rim[x, 2:4] = high_ref[2 * x : 2 * x + 2]
        rim[x, 4:8] = ones

    def along_z(x, _):
        v = jnp.concatenate([eps_ref[x], rim[x]], axis=0)
        h = pltpu.roll(halo[...], lax.rem(254 - 4 * x, 128), 1)
        for ref, value in zip((box, der, inv), zsums(v, h, lane)):
            put(ref, x, value, ny)
        return 0

    lax.fori_loop(0, nx, along_z, 0)

    def along_y(x, _):
        for ref, value in zip((yb, yd, zd, yi), ysums((box, der, inv), x, ny)):
            ref[x] = value
        return 0

    lax.fori_loop(0, nx, along_y, 0)
    for ref, out, wide in ((yb, yb_out, 4), (yd, yd_out, 3), (zd, zd_out, 3), (yi, yi_out, 3)):
        out[0:wide] = ref[0:wide]
        out[wide : 2 * wide] = ref[nx - wide : nx]

    def copy(c):
        return pltpu.make_async_copy(
            obuf.at[:, pl.ds(c * CHUNK, CHUNK)], out_ref.at[:, pl.ds(2 + c * CHUNK, CHUNK)], sem.at[c]
        )

    chunks = (nx - 4) // CHUNK

    def along_x(c, _):
        def one(k, _):
            at = c * CHUNK + k
            x = at + 2
            values = result(
                [yb[x + j] for j in (-2, -1, 0, 1, 2)],
                *[[ref[x + j] for j in (-1, 0, 1)] for ref in (yd, zd, yi)],
            )
            for n, value in enumerate(values):
                obuf[n, at] = value.astype(jnp.bfloat16)
            return 0

        lax.fori_loop(0, CHUNK, one, 0)
        copy(c).start()
        return 0

    lax.fori_loop(0, chunks, along_x, 0)

    def finish(c, _):
        copy(c).wait()
        return 0

    lax.fori_loop(0, chunks, finish, 0)


def outer_kernel(
    low_ref, high_ref, yb_in, yd_in, zd_in, yi_in, _, out_ref,
    box, der, inv, yb, yd, zd, yi, obuf, sem,
):
    nx, ny = out_ref.shape[1], out_ref.shape[2]
    rows = ny + 8
    lane = lanes((rows, 128))
    for k, (ref, s) in enumerate(((low_ref, 0), (low_ref, 1), (high_ref, 0), (high_ref, 1))):
        v = ref[s * rows : (s + 1) * rows]
        packed = ref[2 * rows : 2 * rows + 8]
        h = jnp.concatenate(
            [pltpu.roll(packed, (126 - 8 * g - 4 * s) % 128, 1) for g in range(rows // 8)], axis=0
        )
        for dst, value in zip((box, der, inv), zsums(v, h, lane)):
            put(dst, k, value, ny)
    for k in range(4):
        for ref, value in zip((yb, yd, zd, yi), ysums((box, der, inv), k, ny)):
            ref[k] = value
    for side in range(2):
        for s in range(2):
            def pick(halo_ref, own_ref, wide, j):
                x = s + j
                if side == 0:
                    return halo_ref[2 + x] if x < 0 else own_ref[x]
                x = x - 2
                return halo_ref[2 + x] if x >= 0 else own_ref[2 * wide + x]

            values = result(
                [pick(yb, yb_in, 4, j) for j in (-2, -1, 0, 1, 2)],
                *[[pick(h, o, 3, j) for j in (-1, 0, 1)] for h, o in ((yd, yd_in), (zd, zd_in), (yi, yi_in))],
            )
            for n, value in enumerate(values):
                obuf[n, 2 * side + s] = value.astype(jnp.bfloat16)
        pltpu.make_async_copy(
            obuf.at[:, pl.ds(2 * side, 2)], out_ref.at[:, pl.ds(side * (nx - 2), 2)], sem.at[side]
        ).start()
    for side in range(2):
        pltpu.make_async_copy(
            obuf.at[:, pl.ds(2 * side, 2)], out_ref.at[:, pl.ds(side * (nx - 2), 2)], sem.at[side]
        ).wait()


def cost(us):
    return pl.CostEstimate(flops=int(us * 4e6), bytes_accessed=int(us * 1e6), transcendentals=0)


def shape(*dims, dtype=F32):
    return jax.ShapeDtypeStruct(dims, dtype)


def local(material, eps_table, grading):
    nx, ny, nz = material.shape
    rows = ny + 8
    forward = [(i, (i + 1) % 8) for i in range(8)]
    backward = [(b, a) for a, b in forward]
    even = [(i, i ^ 1) for i in range(8)]
    odd = [((i + 1) % 8, ((i ^ 1) + 1) % 8) for i in range(8)]
    parity = (lax.axis_index("gz") & 1).reshape(1)
    vmem = pltpu.CompilerParams(vmem_limit_bytes=24 << 20)

    y_fwd, y_bwd = pl.pallas_call(
        faces_kernel,
        grid=(1,),
        in_specs=[
            SMEM,
            pl.BlockSpec((nx, 8, nz), lambda i: (0, 0, 0)),
            pl.BlockSpec((nx, 8, nz), lambda i: (0, ny // 8 - 1, 0)),
            pl.BlockSpec((nx, 16, nz), lambda i: (0, 0, 0)),
            pl.BlockSpec((nx, 16, nz), lambda i: (0, ny // 16 - 1, 0)),
        ],
        out_specs=[VMEM, VMEM],
        out_shape=[shape(2 * nx + 8, nz)] * 2,
        compiler_params=vmem,
        cost_estimate=cost(1),
        name="faces",
    )(eps_table, material, material, grading, grading)
    y_low = lax.ppermute(y_fwd, "gy", forward)
    y_high = lax.ppermute(y_bwd, "gy", backward)

    step = 8
    eps, packed = pl.pallas_call(
        block_kernel,
        grid=(nx // step,),
        in_specs=[
            SMEM,
            pl.BlockSpec((step, ny, nz), lambda i: (i, 0, 0)),
            pl.BlockSpec((step, ny, nz), lambda i: (i, 0, 0)),
        ],
        out_specs=[
            pl.BlockSpec((step, ny, nz), lambda i: (i, 0, 0)),
            pl.BlockSpec((ny, nz), lambda i: (0, 0)),
        ],
        out_shape=[shape(nx, ny, nz), shape(ny, nz)],
        compiler_params=vmem,
        cost_estimate=cost(3),
        name="block",
    )(eps_table, material, grading)

    z_face = pl.pallas_call(
        zface_kernel,
        in_specs=[VMEM] * 3,
        out_specs=VMEM,
        out_shape=shape(rows, nz),
        compiler_params=vmem,
        cost_estimate=cost(0.2),
        name="zface",
    )(packed, y_low, y_high)
    z_even = lax.ppermute(z_face, "gz", even)
    z_odd = lax.ppermute(z_face, "gz", odd)

    x_fwd, x_bwd = pl.pallas_call(
        xface_kernel,
        in_specs=[SMEM] + [VMEM] * 5,
        out_specs=[VMEM, VMEM],
        out_shape=[shape(2 * rows + 8, nz)] * 2,
        compiler_params=vmem,
        cost_estimate=cost(0.5),
        name="xface",
    )(parity, eps, y_low, y_high, z_even, z_odd)
    x_low = lax.ppermute(x_fwd, "gx", forward)
    x_high = lax.ppermute(x_bwd, "gx", backward)

    full = (nx, ny + 16, nz)
    out, *edges = pl.pallas_call(
        inner_kernel,
        in_specs=[SMEM] + [VMEM] * 5,
        out_specs=[ANY] + [VMEM] * 4,
        out_shape=[shape(6, nx, ny, nz, dtype=jnp.bfloat16), shape(8, ny, nz)]
        + [shape(6, ny, nz)] * 3,
        scratch_shapes=[
            pltpu.VMEM((nx, 8, nz), F32),
            pltpu.VMEM((rows, nz), F32),
            *[pltpu.VMEM(full, F32)] * 3,
            *[pltpu.VMEM((nx, ny, nz), F32)] * 4,
            pltpu.VMEM((6, nx - 4, ny, nz), jnp.bfloat16),
            pltpu.SemaphoreType.DMA(((nx - 4) // CHUNK,)),
        ],
        compiler_params=vmem,
        cost_estimate=cost(6),
        name="inner",
    )(parity, eps, y_low, y_high, z_even, z_odd)

    return pl.pallas_call(
        outer_kernel,
        in_specs=[VMEM] * 6 + [ANY],
        out_specs=ANY,
        out_shape=shape(6, nx, ny, nz, dtype=jnp.bfloat16),
        input_output_aliases={6: 0},
        scratch_shapes=[
            *[pltpu.VMEM((4, ny + 16, nz), F32)] * 3,
            *[pltpu.VMEM((4, ny, nz), F32)] * 4,
            pltpu.VMEM((6, 4, ny, nz), jnp.bfloat16),
            pltpu.SemaphoreType.DMA((2,)),
        ],
        compiler_params=vmem,
        cost_estimate=cost(1),
        name="outer",
    )(x_low, x_high, *edges, out)


def solution(mesh):
    return jax.shard_map(
        local,
        mesh=mesh,
        in_specs=(P("gx", "gy", "gz"), P(), P("gx", "gy", "gz")),
        out_specs=P(None, "gx", "gy", "gz"),
        check_vma=False,
    )
```

```python
import jax
import jax.numpy as jnp
from jax import lax
from jax.experimental import pallas as pl
from jax.experimental.pallas import tpu as pltpu
from jax.sharding import PartitionSpec as P

F32 = jnp.float32
VMEM = pl.BlockSpec(memory_space=pltpu.VMEM)
SMEM = pl.BlockSpec(memory_space=pltpu.SMEM)
ANY = pl.BlockSpec(memory_space=pl.ANY)
HBM = pl.BlockSpec(memory_space=pltpu.HBM)


def lookup(material, table, grading):
    low = (material & 1) != 0
    mid = (material & 2) != 0
    top = (material & 4) != 0
    pair = [jnp.where(low, table[2 * k + 1], table[2 * k]) for k in range(4)]
    quad = [jnp.where(mid, pair[2 * k + 1], pair[2 * k]) for k in range(2)]
    return jnp.where(top, quad[1], quad[0]) * grading.astype(F32)


def lanes(shape):
    return lax.broadcasted_iota(jnp.int32, shape, len(shape) - 1)


def scalars(table_ref):
    return [table_ref[k] for k in range(8)]


def faces_kernel(
    table_hbm, mat_hbm, gra_hbm, fwd_ref, bwd_ref,
    table_ref, mat_low, mat_high, gra_low, gra_high, sem,
):
    nx, ny = mat_hbm.shape[0], mat_hbm.shape[1]
    copies = [
        pltpu.make_async_copy(src, dst, sem.at[k])
        for k, (src, dst) in enumerate(
            (
                (mat_hbm.at[:, 0:8], mat_low),
                (mat_hbm.at[:, ny - 8 : ny], mat_high),
                (gra_hbm.at[:, 0:16], gra_low),
                (gra_hbm.at[:, ny - 16 : ny], gra_high),
                (table_hbm, table_ref),
            )
        )
    ]
    for copy in copies:
        copy.start()
    for copy in copies:
        copy.wait()
    table = scalars(table_ref)
    lane = lanes((8, 128))
    packed = [jnp.zeros((8, 128), F32)] * 2
    for x in range(nx):
        low = lookup(mat_low[x], table, gra_low[x, 0:8])
        high = lookup(mat_high[x], table, gra_high[x, 8:16])
        bwd_ref[2 * x : 2 * x + 2] = low[0:2]
        fwd_ref[2 * x : 2 * x + 2] = high[6:8]
        here = (lane >> 2) == x
        turn = (4 * x + 2) % 128
        packed = [
            jnp.where(here, pltpu.roll(v, turn, 1) if turn else v, p)
            for v, p in zip((low, high), packed)
        ]
    ones = jnp.ones((6, 128), F32)
    for ref, rows in ((bwd_ref, packed[0][0:2]), (fwd_ref, packed[1][6:8])):
        ref[2 * nx : 2 * nx + 2] = rows
        ref[2 * nx + 2 : 2 * nx + 8] = ones


STEP = 8


def block_kernel(table_hbm, mat_hbm, gra_hbm, eps_ref, packed_ref, table_ref, mat_ref, gra_ref, sem):
    nx, ny = mat_hbm.shape[0], mat_hbm.shape[1]

    def copies(c):
        part = pl.ds(c * STEP, STEP)
        return (
            pltpu.make_async_copy(mat_hbm.at[part], mat_ref.at[part], sem.at[0, c]),
            pltpu.make_async_copy(gra_hbm.at[part], gra_ref.at[part], sem.at[1, c]),
        )

    first = pltpu.make_async_copy(table_hbm, table_ref, sem.at[2, 0])
    first.start()
    for c in range(nx // STEP):
        for copy in copies(c):
            copy.start()
    first.wait()
    table = scalars(table_ref)
    lane = lanes((ny, 128))

    def one(c, packed):
        for copy in copies(c):
            copy.wait()
        for k in range(STEP):
            x = c * STEP + k
            value = lookup(mat_ref[x], table, gra_ref[x])
            eps_ref[x] = value
            packed = jnp.where(
                (lane >> 2) == x, pltpu.roll(value, lax.rem(4 * x + 2, 128), 1), packed
            )
        return packed

    packed_ref[...] = lax.fori_loop(0, nx // STEP, one, jnp.zeros((ny, 128), F32))


def zface_kernel(packed_ref, low_ref, high_ref, out_ref):
    ny = packed_ref.shape[0]
    out_ref[0:ny] = packed_ref[...]
    out_ref[ny : ny + 2] = low_ref[64:66]
    out_ref[ny + 2 : ny + 4] = high_ref[64:66]
    out_ref[ny + 4 : ny + 8] = jnp.ones((4, 128), F32)


def joined(parity_ref, even_ref, odd_ref):
    lane = lanes(even_ref.shape)
    return jnp.where(((lane >> 1) & 1) == parity_ref[0], odd_ref[...], even_ref[...])


def xface_kernel(parity_ref, eps_ref, low_ref, high_ref, even_ref, odd_ref, fwd_ref, bwd_ref):
    nx, ny = eps_ref.shape[0], eps_ref.shape[1]
    rows = ny + 8
    halo = joined(parity_ref, even_ref, odd_ref)
    lane = lanes((8, 128))
    for ref, start in ((fwd_ref, nx - 2), (bwd_ref, 0)):
        for s in range(2):
            x = start + s
            ref[s * rows : s * rows + ny] = eps_ref[x]
            ref[s * rows + ny : s * rows + ny + 2] = low_ref[2 * x : 2 * x + 2]
            ref[s * rows + ny + 2 : s * rows + ny + 4] = high_ref[2 * x : 2 * x + 2]
            ref[s * rows + ny + 4 : s * rows + rows] = jnp.ones((4, 128), F32)
        packed = jnp.ones((8, 128), F32)
        for g in range(rows // 8):
            turn = (8 * g - 4 * start) % 128
            part = halo[8 * g : 8 * g + 8]
            packed = jnp.where((lane >> 3) == g, pltpu.roll(part, turn, 1) if turn else part, packed)
        ref[2 * rows : 2 * rows + 8] = packed


def zsums(v, h, lane):
    left = pltpu.roll(jnp.where(lane == 127, h, v), 1, 1)
    left2 = pltpu.roll(jnp.where(lane >= 126, h, v), 2, 1)
    right = pltpu.roll(jnp.where(lane == 0, h, v), 127, 1)
    right2 = pltpu.roll(jnp.where(lane <= 1, h, v), 126, 1)
    inv, inv_h = 1.0 / v, 1.0 / h
    inv_left = pltpu.roll(jnp.where(lane == 127, inv_h, inv), 1, 1)
    inv_right = pltpu.roll(jnp.where(lane == 0, inv_h, inv), 127, 1)
    return v + left + right, (right + right2) - (left + left2), inv + inv_left + inv_right


def put(ref, index, value, ny):
    ref[index, 8 : 8 + ny] = value[0:ny]
    ref[index, 6:8] = value[ny : ny + 2]
    ref[index, 8 + ny : 10 + ny] = value[ny + 2 : ny + 4]


def ysums(refs, index, count, r):
    box, der, inv = refs
    b = [box[index, 8 + r + k : 8 + r + k + count] for k in (-2, -1, 0, 1, 2)]
    d = [der[index, 8 + r + k : 8 + r + k + count] for k in (-1, 0, 1)]
    i = [inv[index, 8 + r + k : 8 + r + k + count] for k in (-1, 0, 1)]
    return (
        b[1] + b[2] + b[3],
        (b[4] + b[3]) - (b[1] + b[0]),
        d[0] + d[1] + d[2],
        i[0] + i[1] + i[2],
    )


def result(yb, yd, zd, yi):
    mean = yb[1] + yb[2] + yb[3]
    gx = (yb[4] + yb[3]) - (yb[1] + yb[0])
    gy = yd[0] + yd[1] + yd[2]
    gz = zd[0] + zd[1] + zd[2]
    inv = yi[0] + yi[1] + yi[2]
    recip = 27.0 / mean
    factor = (inv * (1.0 / 27.0) - recip) / (gx * gx + gy * gy + gz * gz + 291.6)
    fx, fy, fz = gx * factor, gy * factor, gz * factor
    return (gx * fx + recip, gy * fy + recip, gz * fz + recip, gx * fy, gx * fz, gy * fz)


CHUNK = 4
UNROLL = 4


def inner_kernel(
    parity_ref, eps_ref, low_ref, high_ref, even_ref, odd_ref,
    out_ref, yb_out, yd_out, zd_out, yi_out,
    rim, halo, side, box, der, inv, yb, yd, zd, yi, obuf, sem,
):
    nx, ny = eps_ref.shape[0], eps_ref.shape[1]
    halo[...] = joined(parity_ref, even_ref, odd_ref)
    lane = lanes((ny + 8, 128))
    ones = jnp.ones((4, 128), F32)
    for x in range(nx):
        rim[x, 0:2] = low_ref[2 * x : 2 * x + 2]
        rim[x, 2:4] = high_ref[2 * x : 2 * x + 2]
        rim[x, 4:8] = ones

    def turned(c, _):
        for k in range(UNROLL):
            x = c * UNROLL + k
            side[x] = pltpu.roll(halo[...], lax.rem(254 - 4 * x, 128), 1)
        return 0

    lax.fori_loop(0, nx // UNROLL, turned, 0)

    def along_z(c, _):
        for k in range(UNROLL):
            x = c * UNROLL + k
            v = jnp.concatenate([eps_ref[x], rim[x]], axis=0)
            for ref, value in zip((box, der, inv), zsums(v, side[x], lane)):
                put(ref, x, value, ny)
        return 0

    lax.fori_loop(0, nx // UNROLL, along_z, 0)

    def along_y(x, _):
        for r in range(0, ny, 16):
            for ref, value in zip((yb, yd, zd, yi), ysums((box, der, inv), x, 16, r)):
                ref[x, r : r + 16] = value
        return 0

    lax.fori_loop(0, nx, along_y, 0)
    for ref, out, wide in ((yb, yb_out, 4), (yd, yd_out, 3), (zd, zd_out, 3), (yi, yi_out, 3)):
        out[0:wide] = ref[0:wide]
        out[wide : 2 * wide] = ref[nx - wide : nx]

    def copy(c):
        return pltpu.make_async_copy(
            obuf.at[:, pl.ds(c * CHUNK, CHUNK)], out_ref.at[:, pl.ds(2 + c * CHUNK, CHUNK)], sem.at[c]
        )

    chunks = (nx - 4) // CHUNK

    def along_x(c, _):
        def one(k, _):
            at = c * CHUNK + k
            x = at + 2
            for r in range(0, ny, 16):
                part = slice(r, r + 16)
                values = result(
                    [yb[x + j, part] for j in (-2, -1, 0, 1, 2)],
                    *[[ref[x + j, part] for j in (-1, 0, 1)] for ref in (yd, zd, yi)],
                )
                for n, value in enumerate(values):
                    obuf[n, at, part] = value.astype(jnp.bfloat16)
            return 0

        lax.fori_loop(0, CHUNK, one, 0)
        copy(c).start()
        return 0

    lax.fori_loop(0, chunks, along_x, 0)

    def finish(c, _):
        copy(c).wait()
        return 0

    lax.fori_loop(0, chunks, finish, 0)


def outer_kernel(
    low_ref, high_ref, yb_in, yd_in, zd_in, yi_in, _, out_ref,
    box, der, inv, yb, yd, zd, yi, obuf, sem,
):
    nx, ny = out_ref.shape[1], out_ref.shape[2]
    rows = ny + 8
    lane = lanes((rows, 128))
    for k, (ref, s) in enumerate(((low_ref, 0), (low_ref, 1), (high_ref, 0), (high_ref, 1))):
        v = ref[s * rows : (s + 1) * rows]
        packed = ref[2 * rows : 2 * rows + 8]
        h = jnp.concatenate(
            [pltpu.roll(packed, (126 - 8 * g - 4 * s) % 128, 1) for g in range(rows // 8)], axis=0
        )
        for dst, value in zip((box, der, inv), zsums(v, h, lane)):
            put(dst, k, value, ny)
    for k in range(4):
        for r in range(0, ny, 16):
            for ref, value in zip((yb, yd, zd, yi), ysums((box, der, inv), k, 16, r)):
                ref[k, r : r + 16] = value
    for side in range(2):
        for s in range(2):
            def pick(halo_ref, own_ref, wide, j, part):
                x = s + j
                if side == 0:
                    return halo_ref[2 + x, part] if x < 0 else own_ref[x, part]
                x = x - 2
                return halo_ref[2 + x, part] if x >= 0 else own_ref[2 * wide + x, part]

            for r in range(0, ny, 16):
                part = slice(r, r + 16)
                values = result(
                    [pick(yb, yb_in, 4, j, part) for j in (-2, -1, 0, 1, 2)],
                    *[
                        [pick(h, o, 3, j, part) for j in (-1, 0, 1)]
                        for h, o in ((yd, yd_in), (zd, zd_in), (yi, yi_in))
                    ],
                )
                for n, value in enumerate(values):
                    obuf[n, 2 * side + s, part] = value.astype(jnp.bfloat16)
        pltpu.make_async_copy(
            obuf.at[:, pl.ds(2 * side, 2)], out_ref.at[:, pl.ds(side * (nx - 2), 2)], sem.at[side]
        ).start()
    for side in range(2):
        pltpu.make_async_copy(
            obuf.at[:, pl.ds(2 * side, 2)], out_ref.at[:, pl.ds(side * (nx - 2), 2)], sem.at[side]
        ).wait()


def cost(us):
    return pl.CostEstimate(flops=int(us * 4e6), bytes_accessed=int(us * 1e6), transcendentals=0)


def shape(*dims, dtype=F32):
    return jax.ShapeDtypeStruct(dims, dtype)


def local(material, eps_table, grading):
    nx, ny, nz = material.shape
    rows = ny + 8
    material, eps_table, grading = (
        pltpu.with_memory_space_constraint(a, pltpu.HBM) for a in (material, eps_table, grading)
    )
    forward = [(i, (i + 1) % 8) for i in range(8)]
    backward = [(b, a) for a, b in forward]
    even = [(i, i ^ 1) for i in range(8)]
    odd = [((i + 1) % 8, ((i ^ 1) + 1) % 8) for i in range(8)]
    parity = (lax.axis_index("gz") & 1).reshape(1)
    vmem = pltpu.CompilerParams(vmem_limit_bytes=24 << 20)

    y_fwd, y_bwd = pl.pallas_call(
        faces_kernel,
        in_specs=[HBM] * 3,
        out_specs=[VMEM, VMEM],
        out_shape=[shape(2 * nx + 8, nz)] * 2,
        scratch_shapes=[
            pltpu.SMEM((8,), F32),
            *[pltpu.VMEM((nx, 8, nz), jnp.int32)] * 2,
            *[pltpu.VMEM((nx, 16, nz), jnp.bfloat16)] * 2,
            pltpu.SemaphoreType.DMA((5,)),
        ],
        compiler_params=vmem,
        cost_estimate=cost(1),
        name="faces",
    )(eps_table, material, grading)
    y_low = lax.ppermute(y_fwd, "gy", forward)
    y_high = lax.ppermute(y_bwd, "gy", backward)

    eps, packed = pl.pallas_call(
        block_kernel,
        in_specs=[HBM] * 3,
        out_specs=[VMEM, VMEM],
        out_shape=[shape(nx, ny, nz), shape(ny, nz)],
        scratch_shapes=[
            pltpu.SMEM((8,), F32),
            pltpu.VMEM((nx, ny, nz), jnp.int32),
            pltpu.VMEM((nx, ny, nz), jnp.bfloat16),
            pltpu.SemaphoreType.DMA((3, nx // STEP)),
        ],
        compiler_params=vmem,
        cost_estimate=cost(3),
        name="block",
    )(eps_table, material, grading)

    z_face = pl.pallas_call(
        zface_kernel,
        in_specs=[VMEM] * 3,
        out_specs=VMEM,
        out_shape=shape(rows, nz),
        compiler_params=vmem,
        cost_estimate=cost(0.2),
        name="zface",
    )(packed, y_low, y_high)
    z_even = lax.ppermute(z_face, "gz", even)
    z_odd = lax.ppermute(z_face, "gz", odd)

    x_fwd, x_bwd = pl.pallas_call(
        xface_kernel,
        in_specs=[SMEM] + [VMEM] * 5,
        out_specs=[VMEM, VMEM],
        out_shape=[shape(2 * rows + 8, nz)] * 2,
        compiler_params=vmem,
        cost_estimate=cost(0.5),
        name="xface",
    )(parity, eps, y_low, y_high, z_even, z_odd)
    x_low = lax.ppermute(x_fwd, "gx", forward)
    x_high = lax.ppermute(x_bwd, "gx", backward)

    full = (nx, ny + 16, nz)
    out, *edges = pl.pallas_call(
        inner_kernel,
        in_specs=[SMEM] + [VMEM] * 5,
        out_specs=[ANY] + [VMEM] * 4,
        out_shape=[shape(6, nx, ny, nz, dtype=jnp.bfloat16), shape(8, ny, nz)]
        + [shape(6, ny, nz)] * 3,
        scratch_shapes=[
            pltpu.VMEM((nx, 8, nz), F32),
            pltpu.VMEM((rows, nz), F32),
            pltpu.VMEM((nx, rows, nz), F32),
            *[pltpu.VMEM(full, F32)] * 3,
            *[pltpu.VMEM((nx, ny, nz), F32)] * 4,
            pltpu.VMEM((6, nx - 4, ny, nz), jnp.bfloat16),
            pltpu.SemaphoreType.DMA(((nx - 4) // CHUNK,)),
        ],
        compiler_params=vmem,
        cost_estimate=cost(6),
        name="inner",
    )(parity, eps, y_low, y_high, z_even, z_odd)

    return pl.pallas_call(
        outer_kernel,
        in_specs=[VMEM] * 6 + [ANY],
        out_specs=ANY,
        out_shape=shape(6, nx, ny, nz, dtype=jnp.bfloat16),
        input_output_aliases={6: 0},
        scratch_shapes=[
            *[pltpu.VMEM((4, ny + 16, nz), F32)] * 3,
            *[pltpu.VMEM((4, ny, nz), F32)] * 4,
            pltpu.VMEM((6, 4, ny, nz), jnp.bfloat16),
            pltpu.SemaphoreType.DMA((2,)),
        ],
        compiler_params=vmem,
        cost_estimate=cost(1),
        name="outer",
    )(x_low, x_high, *edges, out)


def solution(mesh):
    return jax.shard_map(
        local,
        mesh=mesh,
        in_specs=(P("gx", "gy", "gz"), P(), P("gx", "gy", "gz")),
        out_specs=P(None, "gx", "gy", "gz"),
        check_vma=False,
    )
```

```python
import jax
import jax.numpy as jnp
from jax import lax
from jax.experimental import pallas as pl
from jax.experimental.pallas import tpu as pltpu
from jax.sharding import PartitionSpec as P

F32 = jnp.float32
VMEM = pl.BlockSpec(memory_space=pltpu.VMEM)
SMEM = pl.BlockSpec(memory_space=pltpu.SMEM)
ANY = pl.BlockSpec(memory_space=pl.ANY)
HBM = pl.BlockSpec(memory_space=pltpu.HBM)


def lookup(material, table, grading):
    low = (material & 1) != 0
    mid = (material & 2) != 0
    top = (material & 4) != 0
    pair = [jnp.where(low, table[2 * k + 1], table[2 * k]) for k in range(4)]
    quad = [jnp.where(mid, pair[2 * k + 1], pair[2 * k]) for k in range(2)]
    return jnp.where(top, quad[1], quad[0]) * grading.astype(F32)


def lanes(shape):
    return lax.broadcasted_iota(jnp.int32, shape, len(shape) - 1)


def scalars(table_ref):
    return [table_ref[k] for k in range(8)]


def finish_face(ref, rows, nx):
    ref[2 * nx : 2 * nx + 2] = rows
    ref[2 * nx + 2 : 2 * nx + 8] = jnp.ones((6, 128), F32)


def face_kernel(
    table_hbm, mat_hbm, gra_hbm, fwd_ref, bwd_ref, mat_ref, gra_ref, rows_ref,
    table_ref, mat_low, mat_high, gra_low, gra_high, sem,
):
    nx, ny = mat_hbm.shape[0], mat_hbm.shape[1]
    copies = [
        pltpu.make_async_copy(src, dst, sem.at[k])
        for k, (src, dst) in enumerate(
            (
                (table_hbm, table_ref),
                (mat_hbm.at[:, 0:8], mat_low),
                (gra_hbm.at[:, 0:16], gra_low),
                (mat_hbm.at[:, ny - 8 : ny], mat_high),
                (gra_hbm.at[:, ny - 16 : ny], gra_high),
                (mat_hbm, mat_ref),
                (gra_hbm, gra_ref),
            )
        )
    ]
    for copy in copies:
        copy.start()
    for copy in copies[:5]:
        copy.wait()
    table = scalars(table_ref)
    for k in range(8):
        rows_ref[k : k + 1] = jnp.full((1, 128), table[k], F32)
    lane = lanes((8, 128))
    packed = [jnp.zeros((8, 128), F32)] * 2
    for x in range(nx):
        low = lookup(mat_low[x], table, gra_low[x, 0:8])
        high = lookup(mat_high[x], table, gra_high[x, 8:16])
        bwd_ref[2 * x : 2 * x + 2] = low[0:2]
        fwd_ref[2 * x : 2 * x + 2] = high[6:8]
        turn = (4 * x + 2) % 128
        packed = [
            jnp.where((lane >> 2) == x, pltpu.roll(v, turn, 1) if turn else v, p)
            for v, p in zip((low, high), packed)
        ]
    finish_face(bwd_ref, packed[0][0:2], nx)
    finish_face(fwd_ref, packed[1][6:8], nx)
    for copy in copies[5:]:
        copy.wait()


STEP = 8


def block_kernel(rows_ref, mat_ref, gra_ref, eps_ref, packed_ref):
    nx, ny = mat_ref.shape[0], mat_ref.shape[1]
    table = [jnp.broadcast_to(rows_ref[k : k + 1], (ny, 128)) for k in range(8)]
    lane = lanes((ny, 128))

    def one(c, packed):
        for k in range(STEP):
            x = c * STEP + k
            value = lookup(mat_ref[x], table, gra_ref[x])
            eps_ref[x] = value
            packed = jnp.where(
                (lane >> 2) == x, pltpu.roll(value, lax.rem(4 * x + 2, 128), 1), packed
            )
        return packed

    packed_ref[...] = lax.fori_loop(0, nx // STEP, one, jnp.zeros((ny, 128), F32))


def zface_kernel(packed_ref, low_ref, high_ref, out_ref):
    ny = packed_ref.shape[0]
    out_ref[0:ny] = packed_ref[...]
    out_ref[ny : ny + 2] = low_ref[64:66]
    out_ref[ny + 2 : ny + 4] = high_ref[64:66]
    out_ref[ny + 4 : ny + 8] = jnp.ones((4, 128), F32)


def joined(parity_ref, even_ref, odd_ref):
    lane = lanes(odd_ref.shape)
    parity = parity_ref[0]
    return jnp.where(((lane >> 1) & 1) == parity, odd_ref[...], even_ref[1 - parity])


def xface_kernel(parity_ref, eps_ref, low_ref, high_ref, even_ref, odd_ref, fwd_ref, bwd_ref):
    nx, ny = eps_ref.shape[0], eps_ref.shape[1]
    rows = ny + 8
    halo = joined(parity_ref, even_ref, odd_ref)
    lane = lanes((8, 128))
    for ref, start in ((fwd_ref, nx - 2), (bwd_ref, 0)):
        for s in range(2):
            x = start + s
            ref[s * rows : s * rows + ny] = eps_ref[x]
            ref[s * rows + ny : s * rows + ny + 2] = low_ref[2 * x : 2 * x + 2]
            ref[s * rows + ny + 2 : s * rows + ny + 4] = high_ref[2 * x : 2 * x + 2]
            ref[s * rows + ny + 4 : s * rows + rows] = jnp.ones((4, 128), F32)
        packed = jnp.ones((8, 128), F32)
        for g in range(rows // 8):
            turn = (8 * g - 4 * start) % 128
            part = halo[8 * g : 8 * g + 8]
            packed = jnp.where((lane >> 3) == g, pltpu.roll(part, turn, 1) if turn else part, packed)
        ref[2 * rows : 2 * rows + 8] = packed


def zsums(v, h, lane):
    left = pltpu.roll(jnp.where(lane == 127, h, v), 1, 1)
    left2 = pltpu.roll(jnp.where(lane >= 126, h, v), 2, 1)
    right = pltpu.roll(jnp.where(lane == 0, h, v), 127, 1)
    right2 = pltpu.roll(jnp.where(lane <= 1, h, v), 126, 1)
    inv, inv_h = 1.0 / v, 1.0 / h
    inv_left = pltpu.roll(jnp.where(lane == 127, inv_h, inv), 1, 1)
    inv_right = pltpu.roll(jnp.where(lane == 0, inv_h, inv), 127, 1)
    return v + left + right, (right + right2) - (left + left2), inv + inv_left + inv_right


def put(ref, index, value, ny):
    ref[index, 8 : 8 + ny] = value[0:ny]
    ref[index, 6:8] = value[ny : ny + 2]
    ref[index, 8 + ny : 10 + ny] = value[ny + 2 : ny + 4]


def ysums(refs, index, count, r):
    box, der, inv = refs
    b = [box[index, 8 + r + k : 8 + r + k + count] for k in (-2, -1, 0, 1, 2)]
    d = [der[index, 8 + r + k : 8 + r + k + count] for k in (-1, 0, 1)]
    i = [inv[index, 8 + r + k : 8 + r + k + count] for k in (-1, 0, 1)]
    return (
        b[1] + b[2] + b[3],
        (b[4] + b[3]) - (b[1] + b[0]),
        d[0] + d[1] + d[2],
        i[0] + i[1] + i[2],
    )


def result(yb, yd, zd, yi):
    mean = yb[1] + yb[2] + yb[3]
    gx = (yb[4] + yb[3]) - (yb[1] + yb[0])
    gy = yd[0] + yd[1] + yd[2]
    gz = zd[0] + zd[1] + zd[2]
    inv = yi[0] + yi[1] + yi[2]
    recip = 27.0 / mean
    factor = (inv * (1.0 / 27.0) - recip) / (gx * gx + gy * gy + gz * gz + 291.6)
    fx, fy, fz = gx * factor, gy * factor, gz * factor
    return (gx * fx + recip, gy * fy + recip, gz * fz + recip, gx * fy, gx * fz, gy * fz)


GROUP = 2
BEHIND = 3 + 4 // GROUP


def inner_kernel(
    parity_ref, eps_ref, low_ref, high_ref, even_ref, odd_ref,
    out_ref, yb, yd, zd, yi, tail,
    rim, halo, side, box, der, inv, obuf, sem,
):
    nx, ny = eps_ref.shape[0], eps_ref.shape[1]
    halo[...] = joined(parity_ref, even_ref, odd_ref)
    lane = lanes((8, 128))
    ones = jnp.ones((4, 128), F32)
    for x in range(nx):
        rim[x, 0:2] = low_ref[2 * x : 2 * x + 2]
        rim[x, 2:4] = high_ref[2 * x : 2 * x + 2]
        rim[x, 4:8] = ones

    def turned(x):
        for r in range(0, ny + 8, 8):
            side[x, r : r + 8] = pltpu.roll(halo[r : r + 8], lax.rem(254 - 4 * x, 128), 1)

    def along_z(x):
        refs = (box, der, inv)
        for r in range(0, ny, 8):
            sums = zsums(eps_ref[x, r : r + 8], side[x, r : r + 8], lane)
            for ref, value in zip(refs, sums):
                ref[x, 8 + r : 16 + r] = value
        for ref, value in zip(refs, zsums(rim[x], side[x, ny : ny + 8], lane)):
            ref[x, 6:8] = value[0:2]
            ref[x, 8 + ny : 10 + ny] = value[2:4]

    def along_y(x):
        for r in range(0, ny, 8):
            for ref, value in zip((yb, yd, zd, yi), ysums((box, der, inv), x, 8, r)):
                ref[x, r : r + 8] = value

    def along_x(x, buffer, at):
        for r in range(0, ny, 16):
            part = slice(r, r + 16)
            values = result(
                [yb[x + j, part] for j in (-2, -1, 0, 1, 2)],
                *[[ref[x + j, part] for j in (-1, 0, 1)] for ref in (yd, zd, yi)],
            )
            for n, value in enumerate(values):
                buffer[n, at, part] = value.astype(jnp.bfloat16)

    def copy(c):
        part = GROUP * c
        return pltpu.make_async_copy(
            obuf.at[:, pl.ds(part, GROUP)], out_ref.at[:, pl.ds(2 + part, GROUP)], sem.at[c]
        )

    groups = nx // GROUP
    last = (nx - 4) // GROUP
    early = groups + 1 - BEHIND
    stages = (
        (turned, 0, groups),
        (along_z, 1, groups),
        (along_y, 2, groups),
        (along_x, BEHIND, last),
    )

    def run(j, active):
        for stage, lag in active:
            for k in range(GROUP):
                x = (j - lag) * GROUP + k
                if stage is not along_x:
                    stage(x)
                elif along_z in [other for other, _ in active]:
                    stage(x + 2, obuf, x)
                else:
                    stage(x + 2, tail, x - early * GROUP)
        if active[0][0] is along_x and along_z in [other for other, _ in active]:
            copy(j - BEHIND).start()

    edges = sorted({lag for _, lag, _ in stages} | {lag + n for _, lag, n in stages})
    for start, stop in zip(edges, edges[1:]):
        active = [(stage, lag) for stage, lag, n in stages[::-1] if lag <= start < lag + n]

        def body(j, carry, active=active):
            run(j, active)
            return carry

        if active:
            lax.fori_loop(start, stop, body, 0)

    def finish(c, carry):
        copy(c).wait()
        return carry

    lax.fori_loop(0, early, finish, 0)


def outer_kernel(
    low_ref, high_ref, yb_in, yd_in, zd_in, yi_in, tail, _, out_ref,
    box, der, inv, yb, yd, zd, yi, obuf, sem,
):
    nx, ny = out_ref.shape[1], out_ref.shape[2]
    rows = ny + 8
    late = pltpu.make_async_copy(
        tail, out_ref.at[:, pl.ds(nx - 2 - tail.shape[1], tail.shape[1])], sem.at[2]
    )
    late.start()
    lane = lanes((rows, 128))
    for k, (ref, s) in enumerate(((low_ref, 0), (low_ref, 1), (high_ref, 0), (high_ref, 1))):
        v = ref[s * rows : (s + 1) * rows]
        packed = ref[2 * rows : 2 * rows + 8]
        h = jnp.concatenate(
            [pltpu.roll(packed, (126 - 8 * g - 4 * s) % 128, 1) for g in range(rows // 8)], axis=0
        )
        for dst, value in zip((box, der, inv), zsums(v, h, lane)):
            put(dst, k, value, ny)
    for k in range(4):
        for r in range(0, ny, 16):
            for ref, value in zip((yb, yd, zd, yi), ysums((box, der, inv), k, 16, r)):
                ref[k, r : r + 16] = value
    for side in range(2):
        for s in range(2):
            def pick(halo_ref, own_ref, j, part):
                x = s + j
                if side == 0:
                    return halo_ref[2 + x, part] if x < 0 else own_ref[x, part]
                x = x - 2
                return halo_ref[2 + x, part] if x >= 0 else own_ref[nx + x, part]

            for r in range(0, ny, 16):
                part = slice(r, r + 16)
                values = result(
                    [pick(yb, yb_in, j, part) for j in (-2, -1, 0, 1, 2)],
                    *[
                        [pick(h, o, j, part) for j in (-1, 0, 1)]
                        for h, o in ((yd, yd_in), (zd, zd_in), (yi, yi_in))
                    ],
                )
                for n, value in enumerate(values):
                    obuf[n, 2 * side + s, part] = value.astype(jnp.bfloat16)
        pltpu.make_async_copy(
            obuf.at[:, pl.ds(2 * side, 2)], out_ref.at[:, pl.ds(side * (nx - 2), 2)], sem.at[side]
        ).start()
    for side in range(2):
        pltpu.make_async_copy(
            obuf.at[:, pl.ds(2 * side, 2)], out_ref.at[:, pl.ds(side * (nx - 2), 2)], sem.at[side]
        ).wait()
    late.wait()


def cost(us):
    return pl.CostEstimate(flops=int(us * 4e6), bytes_accessed=int(us * 1e6), transcendentals=0)


def shape(*dims, dtype=F32):
    return jax.ShapeDtypeStruct(dims, dtype)


def local(material, eps_table, grading):
    nx, ny, nz = material.shape
    rows = ny + 8
    material, eps_table, grading = (
        pltpu.with_memory_space_constraint(a, pltpu.HBM) for a in (material, eps_table, grading)
    )
    forward = [(i, (i + 1) % 8) for i in range(8)]
    backward = [(b, a) for a, b in forward]
    pairs = [[0, 1], [2, 3], [4, 5], [6, 7]]
    odd = [((i + 1) % 8, ((i ^ 1) + 1) % 8) for i in range(8)]
    parity = (lax.axis_index("gz") & 1).reshape(1)
    vmem = pltpu.CompilerParams(vmem_limit_bytes=24 << 20)

    y_face = shape(2 * nx + 8, nz)
    y_fwd, y_bwd, mat_near, gra_near, table_rows = pl.pallas_call(
        face_kernel,
        in_specs=[HBM] * 3,
        out_specs=[VMEM] * 5,
        out_shape=[
            y_face,
            y_face,
            shape(nx, ny, nz, dtype=jnp.int32),
            shape(nx, ny, nz, dtype=jnp.bfloat16),
            shape(8, nz),
        ],
        scratch_shapes=[
            pltpu.SMEM((8,), F32),
            *[pltpu.VMEM((nx, 8, nz), jnp.int32)] * 2,
            *[pltpu.VMEM((nx, 16, nz), jnp.bfloat16)] * 2,
            pltpu.SemaphoreType.DMA((7,)),
        ],
        compiler_params=vmem,
        cost_estimate=cost(1),
        name="face",
    )(eps_table, material, grading)
    y_low = lax.ppermute(y_fwd, "gy", forward)
    y_high = lax.ppermute(y_bwd, "gy", backward)

    eps, packed = pl.pallas_call(
        block_kernel,
        in_specs=[VMEM] * 3,
        out_specs=[VMEM] * 2,
        out_shape=[shape(nx, ny, nz), shape(ny, nz)],
        compiler_params=vmem,
        cost_estimate=cost(3),
        name="block",
    )(table_rows, mat_near, gra_near)

    z_face = pl.pallas_call(
        zface_kernel,
        in_specs=[VMEM] * 3,
        out_specs=VMEM,
        out_shape=shape(rows, nz),
        compiler_params=vmem,
        cost_estimate=cost(0.2),
        name="zface",
    )(packed, y_low, y_high)
    z_odd = lax.ppermute(z_face, "gz", odd)
    z_even = lax.all_gather(z_face, "gz", axis=0, axis_index_groups=pairs)

    x_fwd, x_bwd = pl.pallas_call(
        xface_kernel,
        in_specs=[SMEM] + [VMEM] * 5,
        out_specs=[VMEM, VMEM],
        out_shape=[shape(2 * rows + 8, nz)] * 2,
        compiler_params=vmem,
        cost_estimate=cost(0.5),
        name="xface",
    )(parity, eps, y_low, y_high, z_even, z_odd)
    x_low = lax.ppermute(x_fwd, "gx", forward)
    x_high = lax.ppermute(x_bwd, "gx", backward)

    full = (nx, ny + 16, nz)
    late = nx - 4 - (nx // GROUP + 1 - BEHIND) * GROUP
    out, *edges = pl.pallas_call(
        inner_kernel,
        in_specs=[SMEM] + [VMEM] * 5,
        out_specs=[ANY] + [VMEM] * 5,
        out_shape=[shape(6, nx, ny, nz, dtype=jnp.bfloat16)]
        + [shape(nx, ny, nz)] * 4
        + [shape(6, late, ny, nz, dtype=jnp.bfloat16)],
        scratch_shapes=[
            pltpu.VMEM((nx, 8, nz), F32),
            pltpu.VMEM((rows, nz), F32),
            pltpu.VMEM((nx, rows, nz), F32),
            *[pltpu.VMEM((nx, ny + 16, nz), F32)] * 3,
            pltpu.VMEM((6, nx - 4 - late, ny, nz), jnp.bfloat16),
            pltpu.SemaphoreType.DMA(((nx - 4 - late) // GROUP,)),
        ],
        compiler_params=vmem,
        cost_estimate=cost(6),
        name="inner",
    )(parity, eps, y_low, y_high, z_even, z_odd)

    return pl.pallas_call(
        outer_kernel,
        in_specs=[VMEM] * 7 + [ANY],
        out_specs=ANY,
        out_shape=shape(6, nx, ny, nz, dtype=jnp.bfloat16),
        input_output_aliases={7: 0},
        scratch_shapes=[
            *[pltpu.VMEM((4, ny + 16, nz), F32)] * 3,
            *[pltpu.VMEM((4, ny, nz), F32)] * 4,
            pltpu.VMEM((6, 4, ny, nz), jnp.bfloat16),
            pltpu.SemaphoreType.DMA((3,)),
        ],
        compiler_params=vmem,
        cost_estimate=cost(1),
        name="outer",
    )(x_low, x_high, *edges, out)


def solution(mesh):
    return jax.shard_map(
        local,
        mesh=mesh,
        in_specs=(P("gx", "gy", "gz"), P(), P("gx", "gy", "gz")),
        out_specs=P(None, "gx", "gy", "gz"),
        check_vma=False,
    )
```

```python
import jax
import jax.numpy as jnp
from jax import lax
from jax.experimental import pallas as pl
from jax.experimental.pallas import tpu as pltpu
from jax.sharding import PartitionSpec as P

F32 = jnp.float32
VMEM = pl.BlockSpec(memory_space=pltpu.VMEM)
SMEM = pl.BlockSpec(memory_space=pltpu.SMEM)
ANY = pl.BlockSpec(memory_space=pl.ANY)
HBM = pl.BlockSpec(memory_space=pltpu.HBM)


def lookup(material, table, grading):
    low = (material & 1) != 0
    mid = (material & 2) != 0
    top = (material & 4) != 0
    pair = [jnp.where(low, table[2 * k + 1], table[2 * k]) for k in range(4)]
    quad = [jnp.where(mid, pair[2 * k + 1], pair[2 * k]) for k in range(2)]
    return jnp.where(top, quad[1], quad[0]) * grading.astype(F32)


def lanes(shape):
    return lax.broadcasted_iota(jnp.int32, shape, len(shape) - 1)


def scalars(table_ref):
    return [table_ref[k] for k in range(8)]


def finish_face(ref, rows, nx):
    ref[2 * nx : 2 * nx + 2] = rows
    ref[2 * nx + 2 : 2 * nx + 8] = jnp.ones((6, 128), F32)


def face_kernel(
    table_hbm, mat_hbm, gra_hbm, fwd_ref, bwd_ref, mat_ref, gra_ref, rows_ref, table_ref, sem
):
    nx, ny = mat_hbm.shape[0], mat_hbm.shape[1]
    begin = pltpu.make_async_copy(table_hbm, table_ref, sem.at[2, 0])
    begin.start()
    copies = []
    for c in range(nx // STEP):
        part = slice(c * STEP, (c + 1) * STEP)
        copies.append(
            [
                pltpu.make_async_copy(src.at[part], dst.at[part], sem.at[k, c])
                for k, (src, dst) in enumerate(((mat_hbm, mat_ref), (gra_hbm, gra_ref)))
            ]
        )
        for copy in copies[c]:
            copy.start()
    begin.wait()
    table = scalars(table_ref)
    for k in range(8):
        rows_ref[k : k + 1] = jnp.full((1, 128), table[k], F32)
    lane = lanes((8, 128))
    packed = [jnp.zeros((8, 128), F32)] * 2
    for x in range(nx):
        if x % STEP == 0:
            for copy in copies[x // STEP]:
                copy.wait()
        low = lookup(mat_ref[x, 0:8], table, gra_ref[x, 0:8])
        high = lookup(mat_ref[x, ny - 8 : ny], table, gra_ref[x, ny - 8 : ny])
        bwd_ref[2 * x : 2 * x + 2] = low[0:2]
        fwd_ref[2 * x : 2 * x + 2] = high[6:8]
        turn = (4 * x + 2) % 128
        packed = [
            jnp.where((lane >> 2) == x, pltpu.roll(v, turn, 1) if turn else v, p)
            for v, p in zip((low, high), packed)
        ]
    finish_face(bwd_ref, packed[0][0:2], nx)
    finish_face(fwd_ref, packed[1][6:8], nx)


STEP = 8


def block_kernel(rows_ref, mat_ref, gra_ref, eps_ref, packed_ref):
    nx, ny = mat_ref.shape[0], mat_ref.shape[1]
    table = [jnp.broadcast_to(rows_ref[k : k + 1], (ny, 128)) for k in range(8)]
    lane = lanes((ny, 128))

    def one(c, packed):
        for k in range(STEP):
            x = c * STEP + k
            value = lookup(mat_ref[x], table, gra_ref[x])
            eps_ref[x] = value
            packed = jnp.where(
                (lane >> 2) == x, pltpu.roll(value, lax.rem(4 * x + 2, 128), 1), packed
            )
        return packed

    packed_ref[...] = lax.fori_loop(0, nx // STEP, one, jnp.zeros((ny, 128), F32))


def zface_kernel(packed_ref, low_ref, high_ref, out_ref):
    ny = packed_ref.shape[0]
    out_ref[0:ny] = packed_ref[...]
    out_ref[ny : ny + 2] = low_ref[64:66]
    out_ref[ny + 2 : ny + 4] = high_ref[64:66]
    out_ref[ny + 4 : ny + 8] = jnp.ones((4, 128), F32)


def joined(parity_ref, even_ref, odd_ref):
    lane = lanes(odd_ref.shape)
    parity = parity_ref[0]
    return jnp.where(((lane >> 1) & 1) == parity, odd_ref[...], even_ref[1 - parity])


def xface_kernel(parity_ref, eps_ref, low_ref, high_ref, even_ref, odd_ref, fwd_ref, bwd_ref):
    nx, ny = eps_ref.shape[0], eps_ref.shape[1]
    rows = ny + 8
    halo = joined(parity_ref, even_ref, odd_ref)
    lane = lanes((8, 128))
    for ref, start in ((fwd_ref, nx - 2), (bwd_ref, 0)):
        for s in range(2):
            x = start + s
            ref[s * rows : s * rows + ny] = eps_ref[x]
            ref[s * rows + ny : s * rows + ny + 2] = low_ref[2 * x : 2 * x + 2]
            ref[s * rows + ny + 2 : s * rows + ny + 4] = high_ref[2 * x : 2 * x + 2]
            ref[s * rows + ny + 4 : s * rows + rows] = jnp.ones((4, 128), F32)
        packed = jnp.ones((8, 128), F32)
        for g in range(rows // 8):
            turn = (8 * g - 4 * start) % 128
            part = halo[8 * g : 8 * g + 8]
            packed = jnp.where((lane >> 3) == g, pltpu.roll(part, turn, 1) if turn else part, packed)
        ref[2 * rows : 2 * rows + 8] = packed


def zsums(v, h, lane):
    left = pltpu.roll(jnp.where(lane == 127, h, v), 1, 1)
    left2 = pltpu.roll(jnp.where(lane >= 126, h, v), 2, 1)
    right = pltpu.roll(jnp.where(lane == 0, h, v), 127, 1)
    right2 = pltpu.roll(jnp.where(lane <= 1, h, v), 126, 1)
    inv, inv_h = 1.0 / v, 1.0 / h
    inv_left = pltpu.roll(jnp.where(lane == 127, inv_h, inv), 1, 1)
    inv_right = pltpu.roll(jnp.where(lane == 0, inv_h, inv), 127, 1)
    return v + left + right, (right + right2) - (left + left2), inv + inv_left + inv_right


def inverse_zsum(v, h, lane):
    inv, inv_h = 1.0 / v, 1.0 / h
    inv_left = pltpu.roll(jnp.where(lane == 127, inv_h, inv), 1, 1)
    inv_right = pltpu.roll(jnp.where(lane == 0, inv_h, inv), 127, 1)
    return inv + inv_left + inv_right


def tap_matrix():
    shape = (512, 256)
    row = lax.broadcasted_iota(jnp.int32, shape, 0) & 255
    column = lax.broadcasted_iota(jnp.int32, shape, 1)
    place = jnp.where(row < 128, row, jnp.where(row >= 192, row - 256, row))
    away = place - (column & 127)
    box = jnp.where(jnp.abs(away) <= 1, 1.0, 0.0)
    outer = jnp.where((jnp.abs(away) == 1) | (jnp.abs(away) == 2), 1.0, 0.0)
    der = jnp.where(away > 0, outer, -outer)
    return jnp.where(column < 128, box, der).astype(jnp.bfloat16)


def put(ref, index, value, ny):
    ref[index, 8 : 8 + ny] = value[0:ny]
    ref[index, 6:8] = value[ny : ny + 2]
    ref[index, 8 + ny : 10 + ny] = value[ny + 2 : ny + 4]


def ysums(refs, index, count, r):
    box, der, inv = refs
    b = [box[index, 8 + r + k : 8 + r + k + count] for k in (-2, -1, 0, 1, 2)]
    d = [der[index, 8 + r + k : 8 + r + k + count] for k in (-1, 0, 1)]
    i = [inv[index, 8 + r + k : 8 + r + k + count] for k in (-1, 0, 1)]
    return (
        b[1] + b[2] + b[3],
        (b[4] + b[3]) - (b[1] + b[0]),
        d[0] + d[1] + d[2],
        i[0] + i[1] + i[2],
    )


def result(yb, yd, zd, yi):
    mean = yb[1] + yb[2] + yb[3]
    gx = (yb[4] + yb[3]) - (yb[1] + yb[0])
    gy = yd[0] + yd[1] + yd[2]
    gz = zd[0] + zd[1] + zd[2]
    inv = yi[0] + yi[1] + yi[2]
    recip = 27.0 / mean
    factor = (inv * (1.0 / 27.0) - recip) / (gx * gx + gy * gy + gz * gz + 291.6)
    fx, fy, fz = gx * factor, gy * factor, gz * factor
    return (gx * fx + recip, gy * fy + recip, gz * fz + recip, gx * fy, gx * fz, gy * fz)


GROUP = 4
BEHIND = 3 + 4 // GROUP


def inner_kernel(
    parity_ref, eps_ref, low_ref, high_ref, even_ref, odd_ref,
    out_ref, yb, yd, zd, yi, tail,
    rim, halo, side, taps, box, der, inv, obuf, sem,
):
    nx, ny = eps_ref.shape[0], eps_ref.shape[1]
    halo[...] = joined(parity_ref, even_ref, odd_ref)
    taps[...] = tap_matrix()
    lane = lanes((8, 128))
    ones = jnp.ones((4, 128), F32)
    for x in range(nx):
        rim[x, 0:2] = low_ref[2 * x : 2 * x + 2]
        rim[x, 2:4] = high_ref[2 * x : 2 * x + 2]
        rim[x, 4:8] = ones

    def turned(x):
        for r in range(0, ny + 8, 8):
            side[x, r : r + 8] = pltpu.roll(halo[r : r + 8], lax.rem(254 - 4 * x, 128), 1)

    def along_z(c):
        slices = range(GROUP)
        for k in slices:
            x = c * GROUP + k
            for r in range(0, ny, 8):
                value = inverse_zsum(eps_ref[x, r : r + 8], side[x, r : r + 8], lane)
                inv[x, 8 + r : 16 + r] = value
            value = inverse_zsum(rim[x], side[x, ny : ny + 8], lane)
            inv[x, 6:8] = value[0:2]
            inv[x, 8 + ny : 10 + ny] = value[2:4]
        own = jnp.concatenate(
            [part for k in slices for part in (eps_ref[c * GROUP + k], rim[c * GROUP + k])], axis=0
        )
        near = jnp.concatenate([side[c * GROUP + k] for k in slices], axis=0)
        values = jnp.concatenate([own, near], axis=1)
        coarse = values.astype(jnp.bfloat16)
        fine = (values - coarse.astype(F32)).astype(jnp.bfloat16)
        sums = jnp.dot(
            jnp.concatenate([coarse, fine], axis=1), taps[...], preferred_element_type=F32
        )
        for ref, part in ((box, sums[:, 0:128]), (der, sums[:, 128:256])):
            for k in slices:
                x, at = c * GROUP + k, k * (ny + 8)
                ref[x, 8 : 8 + ny] = part[at : at + ny]
                ref[x, 6:8] = part[at + ny : at + ny + 2]
                ref[x, 8 + ny : 10 + ny] = part[at + ny + 2 : at + ny + 4]

    def along_y(x):
        for r in range(0, ny, 8):
            for ref, value in zip((yb, yd, zd, yi), ysums((box, der, inv), x, 8, r)):
                ref[x, r : r + 8] = value

    def along_x(x, buffer, at):
        for r in range(0, ny, 16):
            part = slice(r, r + 16)
            values = result(
                [yb[x + j, part] for j in (-2, -1, 0, 1, 2)],
                *[[ref[x + j, part] for j in (-1, 0, 1)] for ref in (yd, zd, yi)],
            )
            for n, value in enumerate(values):
                buffer[n, at, part] = value.astype(jnp.bfloat16)

    def copy(c):
        part = GROUP * c
        return pltpu.make_async_copy(
            obuf.at[:, pl.ds(part, GROUP)], out_ref.at[:, pl.ds(2 + part, GROUP)], sem.at[c]
        )

    groups = nx // GROUP
    last = (nx - 4) // GROUP
    early = groups + 1 - BEHIND
    stages = (
        (turned, 0, groups),
        (along_z, 1, groups),
        (along_y, 2, groups),
        (along_x, BEHIND, last),
    )

    def run(j, active):
        for stage, lag in active:
            if stage is along_z:
                stage(j - lag)
                continue
            for k in range(GROUP):
                x = (j - lag) * GROUP + k
                if stage is not along_x:
                    stage(x)
                elif along_z in [other for other, _ in active]:
                    stage(x + 2, obuf, x)
                else:
                    stage(x + 2, tail, x - early * GROUP)
        if active[0][0] is along_x and along_z in [other for other, _ in active]:
            copy(j - BEHIND).start()

    edges = sorted({lag for _, lag, _ in stages} | {lag + n for _, lag, n in stages})
    for start, stop in zip(edges, edges[1:]):
        active = [(stage, lag) for stage, lag, n in stages[::-1] if lag <= start < lag + n]

        def body(j, carry, active=active):
            run(j, active)
            return carry

        if active:
            lax.fori_loop(start, stop, body, 0)

    def finish(c, carry):
        copy(c).wait()
        return carry

    lax.fori_loop(0, early, finish, 0)


def outer_kernel(
    low_ref, high_ref, yb_in, yd_in, zd_in, yi_in, tail, _, out_ref,
    box, der, inv, yb, yd, zd, yi, obuf, sem,
):
    nx, ny = out_ref.shape[1], out_ref.shape[2]
    rows = ny + 8
    late = pltpu.make_async_copy(
        tail, out_ref.at[:, pl.ds(nx - 2 - tail.shape[1], tail.shape[1])], sem.at[4]
    )
    late.start()

    def finish(k):
        x = k if k < 2 else nx - 4 + k
        return pltpu.make_async_copy(
            obuf.at[:, pl.ds(k, 1)], out_ref.at[:, pl.ds(x, 1)], sem.at[k]
        )

    lane = lanes((rows, 128))
    for k, (ref, s) in enumerate(((low_ref, 0), (low_ref, 1), (high_ref, 0), (high_ref, 1))):
        v = ref[s * rows : (s + 1) * rows]
        packed = ref[2 * rows : 2 * rows + 8]
        h = jnp.concatenate(
            [pltpu.roll(packed, (126 - 8 * g - 4 * s) % 128, 1) for g in range(rows // 8)], axis=0
        )
        for dst, value in zip((box, der, inv), zsums(v, h, lane)):
            put(dst, k, value, ny)
    for k in range(4):
        for r in range(0, ny, 16):
            for ref, value in zip((yb, yd, zd, yi), ysums((box, der, inv), k, 16, r)):
                ref[k, r : r + 16] = value
    for side in range(2):
        for s in range(2):
            def pick(halo_ref, own_ref, j, part):
                x = s + j
                if side == 0:
                    return halo_ref[2 + x, part] if x < 0 else own_ref[x, part]
                x = x - 2
                return halo_ref[2 + x, part] if x >= 0 else own_ref[nx + x, part]

            for r in range(0, ny, 16):
                part = slice(r, r + 16)
                values = result(
                    [pick(yb, yb_in, j, part) for j in (-2, -1, 0, 1, 2)],
                    *[
                        [pick(h, o, j, part) for j in (-1, 0, 1)]
                        for h, o in ((yd, yd_in), (zd, zd_in), (yi, yi_in))
                    ],
                )
                for n, value in enumerate(values):
                    obuf[n, 2 * side + s, part] = value.astype(jnp.bfloat16)
            finish(2 * side + s).start()
    for k in range(4):
        finish(k).wait()
    late.wait()


def cost(us):
    return pl.CostEstimate(flops=int(us * 4e6), bytes_accessed=int(us * 1e6), transcendentals=0)


def shape(*dims, dtype=F32):
    return jax.ShapeDtypeStruct(dims, dtype)


def local(material, eps_table, grading):
    nx, ny, nz = material.shape
    rows = ny + 8
    material, eps_table, grading = (
        pltpu.with_memory_space_constraint(a, pltpu.HBM) for a in (material, eps_table, grading)
    )
    forward = [(i, (i + 1) % 8) for i in range(8)]
    backward = [(b, a) for a, b in forward]
    pairs = [[0, 1], [2, 3], [4, 5], [6, 7]]
    odd = [((i + 1) % 8, ((i ^ 1) + 1) % 8) for i in range(8)]
    parity = (lax.axis_index("gz") & 1).reshape(1)
    vmem = pltpu.CompilerParams(vmem_limit_bytes=24 << 20)

    y_face = shape(2 * nx + 8, nz)
    y_fwd, y_bwd, mat_near, gra_near, table_rows = pl.pallas_call(
        face_kernel,
        in_specs=[HBM] * 3,
        out_specs=[VMEM] * 5,
        out_shape=[
            y_face,
            y_face,
            shape(nx, ny, nz, dtype=jnp.int32),
            shape(nx, ny, nz, dtype=jnp.bfloat16),
            shape(8, nz),
        ],
        scratch_shapes=[
            pltpu.SMEM((8,), F32),
            pltpu.SemaphoreType.DMA((3, nx // STEP)),
        ],
        compiler_params=vmem,
        cost_estimate=cost(1),
        name="face",
    )(eps_table, material, grading)
    y_low = lax.ppermute(y_fwd, "gy", forward)
    y_high = lax.ppermute(y_bwd, "gy", backward)

    eps, packed = pl.pallas_call(
        block_kernel,
        in_specs=[VMEM] * 3,
        out_specs=[VMEM] * 2,
        out_shape=[shape(nx, ny, nz), shape(ny, nz)],
        compiler_params=vmem,
        cost_estimate=cost(3),
        name="block",
    )(table_rows, mat_near, gra_near)

    z_face = pl.pallas_call(
        zface_kernel,
        in_specs=[VMEM] * 3,
        out_specs=VMEM,
        out_shape=shape(rows, nz),
        compiler_params=vmem,
        cost_estimate=cost(0.2),
        name="zface",
    )(packed, y_low, y_high)
    z_odd = lax.ppermute(z_face, "gz", odd)
    z_even = lax.all_gather(z_face, "gz", axis=0, axis_index_groups=pairs)

    x_fwd, x_bwd = pl.pallas_call(
        xface_kernel,
        in_specs=[SMEM] + [VMEM] * 5,
        out_specs=[VMEM, VMEM],
        out_shape=[shape(2 * rows + 8, nz)] * 2,
        compiler_params=vmem,
        cost_estimate=cost(0.5),
        name="xface",
    )(parity, eps, y_low, y_high, z_even, z_odd)
    x_low = lax.ppermute(x_fwd, "gx", forward)
    x_high = lax.ppermute(x_bwd, "gx", backward)

    full = (nx, ny + 16, nz)
    late = nx - 4 - (nx // GROUP + 1 - BEHIND) * GROUP
    out, *edges = pl.pallas_call(
        inner_kernel,
        in_specs=[SMEM] + [VMEM] * 5,
        out_specs=[ANY] + [VMEM] * 5,
        out_shape=[shape(6, nx, ny, nz, dtype=jnp.bfloat16)]
        + [shape(nx, ny, nz)] * 4
        + [shape(6, late, ny, nz, dtype=jnp.bfloat16)],
        scratch_shapes=[
            pltpu.VMEM((nx, 8, nz), F32),
            pltpu.VMEM((rows, nz), F32),
            pltpu.VMEM((nx, rows, nz), F32),
            pltpu.VMEM((512, 256), jnp.bfloat16),
            *[pltpu.VMEM((nx, ny + 16, nz), F32)] * 3,
            pltpu.VMEM((6, nx - 4 - late, ny, nz), jnp.bfloat16),
            pltpu.SemaphoreType.DMA(((nx - 4 - late) // GROUP,)),
        ],
        compiler_params=vmem,
        cost_estimate=cost(6),
        name="inner",
    )(parity, eps, y_low, y_high, z_even, z_odd)

    return pl.pallas_call(
        outer_kernel,
        in_specs=[VMEM] * 7 + [ANY],
        out_specs=ANY,
        out_shape=shape(6, nx, ny, nz, dtype=jnp.bfloat16),
        input_output_aliases={7: 0},
        scratch_shapes=[
            *[pltpu.VMEM((4, ny + 16, nz), F32)] * 3,
            *[pltpu.VMEM((4, ny, nz), F32)] * 4,
            pltpu.VMEM((6, 4, ny, nz), jnp.bfloat16),
            pltpu.SemaphoreType.DMA((5,)),
        ],
        compiler_params=vmem,
        cost_estimate=cost(1),
        name="outer",
    )(x_low, x_high, *edges, out)


def solution(mesh):
    return jax.shard_map(
        local,
        mesh=mesh,
        in_specs=(P("gx", "gy", "gz"), P(), P("gx", "gy", "gz")),
        out_specs=P(None, "gx", "gy", "gz"),
        check_vma=False,
    )
```

```python
import jax
import jax.numpy as jnp
from jax import lax
from jax.experimental import pallas as pl
from jax.experimental.pallas import tpu as pltpu
from jax.sharding import PartitionSpec as P

F32 = jnp.float32
VMEM = pl.BlockSpec(memory_space=pltpu.VMEM)
SMEM = pl.BlockSpec(memory_space=pltpu.SMEM)
ANY = pl.BlockSpec(memory_space=pl.ANY)
HBM = pl.BlockSpec(memory_space=pltpu.HBM)


def lookup(material, table, grading):
    low = (material & 1) != 0
    mid = (material & 2) != 0
    top = (material & 4) != 0
    pair = [jnp.where(low, table[2 * k + 1], table[2 * k]) for k in range(4)]
    quad = [jnp.where(mid, pair[2 * k + 1], pair[2 * k]) for k in range(2)]
    return jnp.where(top, quad[1], quad[0]) * grading.astype(F32)


def lanes(shape):
    return lax.broadcasted_iota(jnp.int32, shape, len(shape) - 1)


def scalars(table_ref):
    return [table_ref[k] for k in range(8)]


def finish_face(ref, rows, nx):
    ref[2 * nx : 2 * nx + 2] = rows
    ref[2 * nx + 2 : 2 * nx + 8] = jnp.ones((6, 128), F32)


def face_kernel(
    table_hbm, mat_hbm, gra_hbm, fwd_ref, bwd_ref, mat_ref, gra_ref, rows_ref, table_ref, sem
):
    nx, ny = mat_hbm.shape[0], mat_hbm.shape[1]
    begin = pltpu.make_async_copy(table_hbm, table_ref, sem.at[2, 0])
    begin.start()
    copies = []
    for c in range(nx // STEP):
        part = slice(c * STEP, (c + 1) * STEP)
        copies.append(
            [
                pltpu.make_async_copy(src.at[part], dst.at[part], sem.at[k, c])
                for k, (src, dst) in enumerate(((mat_hbm, mat_ref), (gra_hbm, gra_ref)))
            ]
        )
        for copy in copies[c]:
            copy.start()
    begin.wait()
    table = scalars(table_ref)
    for k in range(8):
        rows_ref[k : k + 1] = jnp.full((1, 128), table[k], F32)
    lane = lanes((8, 128))
    packed = [jnp.zeros((8, 128), F32)] * 2
    for x in range(nx):
        if x % STEP == 0:
            for copy in copies[x // STEP]:
                copy.wait()
        low = lookup(mat_ref[x, 0:8], table, gra_ref[x, 0:8])
        high = lookup(mat_ref[x, ny - 8 : ny], table, gra_ref[x, ny - 8 : ny])
        bwd_ref[2 * x : 2 * x + 2] = low[0:2]
        fwd_ref[2 * x : 2 * x + 2] = high[6:8]
        turn = (4 * x + 2) % 128
        packed = [
            jnp.where((lane >> 2) == x, pltpu.roll(v, turn, 1) if turn else v, p)
            for v, p in zip((low, high), packed)
        ]
    finish_face(bwd_ref, packed[0][0:2], nx)
    finish_face(fwd_ref, packed[1][6:8], nx)


STEP = 8


def block_kernel(rows_ref, mat_ref, gra_ref, eps_ref, packed_ref):
    nx, ny = mat_ref.shape[0], mat_ref.shape[1]
    table = [jnp.broadcast_to(rows_ref[k : k + 1], (ny, 128)) for k in range(8)]
    lane = lanes((ny, 128))

    def one(c, packed):
        for k in range(STEP):
            x = c * STEP + k
            value = lookup(mat_ref[x], table, gra_ref[x])
            eps_ref[x] = value
            packed = jnp.where(
                (lane >> 2) == x, pltpu.roll(value, lax.rem(4 * x + 2, 128), 1), packed
            )
        return packed

    packed_ref[...] = lax.fori_loop(0, nx // STEP, one, jnp.zeros((ny, 128), F32))


def zface_kernel(packed_ref, low_ref, high_ref, out_ref):
    ny = packed_ref.shape[0]
    out_ref[0:ny] = packed_ref[...]
    out_ref[ny : ny + 2] = low_ref[64:66]
    out_ref[ny + 2 : ny + 4] = high_ref[64:66]
    out_ref[ny + 4 : ny + 8] = jnp.ones((4, 128), F32)


def joined(parity_ref, even_ref, odd_ref):
    lane = lanes(odd_ref.shape)
    parity = parity_ref[0]
    return jnp.where(((lane >> 1) & 1) == parity, odd_ref[...], even_ref[1 - parity])


def xface_kernel(parity_ref, eps_ref, low_ref, high_ref, even_ref, odd_ref, fwd_ref, bwd_ref):
    nx, ny = eps_ref.shape[0], eps_ref.shape[1]
    rows = ny + 8
    halo = joined(parity_ref, even_ref, odd_ref)
    lane = lanes((8, 128))
    for ref, start in ((fwd_ref, nx - 2), (bwd_ref, 0)):
        for s in range(2):
            x = start + s
            ref[s * rows : s * rows + ny] = eps_ref[x]
            ref[s * rows + ny : s * rows + ny + 2] = low_ref[2 * x : 2 * x + 2]
            ref[s * rows + ny + 2 : s * rows + ny + 4] = high_ref[2 * x : 2 * x + 2]
            ref[s * rows + ny + 4 : s * rows + rows] = jnp.ones((4, 128), F32)
        packed = jnp.ones((8, 128), F32)
        for g in range(rows // 8):
            turn = (8 * g - 4 * start) % 128
            part = halo[8 * g : 8 * g + 8]
            packed = jnp.where((lane >> 3) == g, pltpu.roll(part, turn, 1) if turn else part, packed)
        ref[2 * rows : 2 * rows + 8] = packed


def zsums(v, h, lane):
    left = pltpu.roll(jnp.where(lane == 127, h, v), 1, 1)
    left2 = pltpu.roll(jnp.where(lane >= 126, h, v), 2, 1)
    right = pltpu.roll(jnp.where(lane == 0, h, v), 127, 1)
    right2 = pltpu.roll(jnp.where(lane <= 1, h, v), 126, 1)
    inv, inv_h = 1.0 / v, 1.0 / h
    inv_left = pltpu.roll(jnp.where(lane == 127, inv_h, inv), 1, 1)
    inv_right = pltpu.roll(jnp.where(lane == 0, inv_h, inv), 127, 1)
    return v + left + right, (right + right2) - (left + left2), inv + inv_left + inv_right


def inverse_zsum(v, h, lane):
    inv, inv_h = 1.0 / v, 1.0 / h
    inv_left = pltpu.roll(jnp.where(lane == 127, inv_h, inv), 1, 1)
    inv_right = pltpu.roll(jnp.where(lane == 0, inv_h, inv), 127, 1)
    return inv + inv_left + inv_right


def tap_matrix():
    shape = (512, 256)
    row = lax.broadcasted_iota(jnp.int32, shape, 0) & 255
    column = lax.broadcasted_iota(jnp.int32, shape, 1)
    place = jnp.where(row < 128, row, jnp.where(row >= 192, row - 256, row))
    away = place - (column & 127)
    box = jnp.where(jnp.abs(away) <= 1, 1.0, 0.0)
    outer = jnp.where((jnp.abs(away) == 1) | (jnp.abs(away) == 2), 1.0, 0.0)
    der = jnp.where(away > 0, outer, -outer)
    return jnp.where(column < 128, box, der).astype(jnp.bfloat16)


def put(ref, index, value, ny):
    ref[index, 8 : 8 + ny] = value[0:ny]
    ref[index, 6:8] = value[ny : ny + 2]
    ref[index, 8 + ny : 10 + ny] = value[ny + 2 : ny + 4]


def ysums(refs, index, count, r):
    box, der, inv = refs
    b = [box[index, 8 + r + k : 8 + r + k + count] for k in (-2, -1, 0, 1, 2)]
    d = [der[index, 8 + r + k : 8 + r + k + count] for k in (-1, 0, 1)]
    i = [inv[index, 8 + r + k : 8 + r + k + count] for k in (-1, 0, 1)]
    return (
        b[1] + b[2] + b[3],
        (b[4] + b[3]) - (b[1] + b[0]),
        d[0] + d[1] + d[2],
        i[0] + i[1] + i[2],
    )


def result(yb, yd, zd, yi):
    mean = yb[1] + yb[2] + yb[3]
    gx = (yb[4] + yb[3]) - (yb[1] + yb[0])
    gy = yd[0] + yd[1] + yd[2]
    gz = zd[0] + zd[1] + zd[2]
    inv = yi[0] + yi[1] + yi[2]
    recip = 27.0 / mean
    factor = (inv * (1.0 / 27.0) - recip) / (gx * gx + gy * gy + gz * gz + 291.6)
    fx, fy, fz = gx * factor, gy * factor, gz * factor
    return (gx * fx + recip, gy * fy + recip, gz * fz + recip, gx * fy, gx * fz, gy * fz)


GROUP = 4
BEHIND = 3 + 4 // GROUP
EARLY = 3


def inner_kernel(
    parity_ref, eps_ref, low_ref, high_ref, even_ref, odd_ref,
    out_ref, yb, yd, zd, yi, tail,
    rim, halo, side, taps, box, der, inv, obuf, sem,
):
    nx, ny = eps_ref.shape[0], eps_ref.shape[1]
    halo[...] = joined(parity_ref, even_ref, odd_ref)
    taps[...] = tap_matrix()
    lane = lanes((8, 128))
    ones = jnp.ones((4, 128), F32)
    for x in range(nx):
        rim[x, 0:2] = low_ref[2 * x : 2 * x + 2]
        rim[x, 2:4] = high_ref[2 * x : 2 * x + 2]
        rim[x, 4:8] = ones

    def turned(x):
        for r in range(0, ny + 8, 8):
            side[x, r : r + 8] = pltpu.roll(halo[r : r + 8], lax.rem(254 - 4 * x, 128), 1)

    def along_z(c):
        slices = range(GROUP)
        for k in slices:
            x = c * GROUP + k
            for r in range(0, ny, 8):
                value = inverse_zsum(eps_ref[x, r : r + 8], side[x, r : r + 8], lane)
                inv[x, 8 + r : 16 + r] = value
            value = inverse_zsum(rim[x], side[x, ny : ny + 8], lane)
            inv[x, 6:8] = value[0:2]
            inv[x, 8 + ny : 10 + ny] = value[2:4]
        own = jnp.concatenate(
            [part for k in slices for part in (eps_ref[c * GROUP + k], rim[c * GROUP + k])], axis=0
        )
        near = jnp.concatenate([side[c * GROUP + k] for k in slices], axis=0)
        values = jnp.concatenate([own, near], axis=1)
        coarse = values.astype(jnp.bfloat16)
        fine = (values - coarse.astype(F32)).astype(jnp.bfloat16)
        sums = jnp.dot(
            jnp.concatenate([coarse, fine], axis=1), taps[...], preferred_element_type=F32
        )
        for ref, part in ((box, sums[:, 0:128]), (der, sums[:, 128:256])):
            for k in slices:
                x, at = c * GROUP + k, k * (ny + 8)
                ref[x, 8 : 8 + ny] = part[at : at + ny]
                ref[x, 6:8] = part[at + ny : at + ny + 2]
                ref[x, 8 + ny : 10 + ny] = part[at + ny + 2 : at + ny + 4]

    def along_y(x):
        for r in range(0, ny, 8):
            for ref, value in zip((yb, yd, zd, yi), ysums((box, der, inv), x, 8, r)):
                ref[x, r : r + 8] = value

    def along_x(x, buffer, at):
        for r in range(0, ny, 16):
            part = slice(r, r + 16)
            values = result(
                [yb[x + j, part] for j in (-2, -1, 0, 1, 2)],
                *[[ref[x + j, part] for j in (-1, 0, 1)] for ref in (yd, zd, yi)],
            )
            for n, value in enumerate(values):
                buffer[n, at, part] = value.astype(jnp.bfloat16)

    def copy(c):
        part = GROUP * c
        return pltpu.make_async_copy(
            obuf.at[:, pl.ds(part, GROUP)], out_ref.at[:, pl.ds(2 + part, GROUP)], sem.at[c]
        )

    groups = nx // GROUP
    last = (nx - 4) // GROUP
    early = EARLY
    stages = (
        (turned, 0, groups),
        (along_z, 1, groups),
        (along_y, 2, groups),
        (along_x, BEHIND, last),
    )

    def run(j, active, soon):
        for stage, lag in active:
            if stage is along_z:
                stage(j - lag)
                continue
            for k in range(GROUP):
                x = (j - lag) * GROUP + k
                if stage is not along_x:
                    stage(x)
                elif soon:
                    stage(x + 2, obuf, x)
                else:
                    stage(x + 2, tail, x - early * GROUP)
        if active[0][0] is along_x and soon:
            copy(j - BEHIND).start()

    edges = sorted(
        {lag for _, lag, _ in stages} | {lag + n for _, lag, n in stages} | {BEHIND + early}
    )
    for start, stop in zip(edges, edges[1:]):
        active = [(stage, lag) for stage, lag, n in stages[::-1] if lag <= start < lag + n]

        def body(j, carry, active=active, soon=start < BEHIND + early):
            run(j, active, soon)
            return carry

        if active:
            lax.fori_loop(start, stop, body, 0)

    def finish(c, carry):
        copy(c).wait()
        return carry

    lax.fori_loop(0, early, finish, 0)


def outer_kernel(
    low_ref, high_ref, yb_in, yd_in, zd_in, yi_in, tail, _, out_ref,
    box, der, inv, yb, yd, zd, yi, obuf, sem,
):
    nx, ny = out_ref.shape[1], out_ref.shape[2]
    rows = ny + 8
    late = pltpu.make_async_copy(
        tail, out_ref.at[:, pl.ds(nx - 2 - tail.shape[1], tail.shape[1])], sem.at[4]
    )
    late.start()

    def finish(k):
        x = k if k < 2 else nx - 4 + k
        return pltpu.make_async_copy(
            obuf.at[:, pl.ds(k, 1)], out_ref.at[:, pl.ds(x, 1)], sem.at[k]
        )

    lane = lanes((rows, 128))
    for k, (ref, s) in enumerate(((low_ref, 0), (low_ref, 1), (high_ref, 0), (high_ref, 1))):
        v = ref[s * rows : (s + 1) * rows]
        packed = ref[2 * rows : 2 * rows + 8]
        h = jnp.concatenate(
            [pltpu.roll(packed, (126 - 8 * g - 4 * s) % 128, 1) for g in range(rows // 8)], axis=0
        )
        for dst, value in zip((box, der, inv), zsums(v, h, lane)):
            put(dst, k, value, ny)
    for k in range(4):
        for r in range(0, ny, 16):
            for ref, value in zip((yb, yd, zd, yi), ysums((box, der, inv), k, 16, r)):
                ref[k, r : r + 16] = value
    for side in range(2):
        for s in range(2):
            def pick(halo_ref, own_ref, j, part):
                x = s + j
                if side == 0:
                    return halo_ref[2 + x, part] if x < 0 else own_ref[x, part]
                x = x - 2
                return halo_ref[2 + x, part] if x >= 0 else own_ref[nx + x, part]

            for r in range(0, ny, 16):
                part = slice(r, r + 16)
                values = result(
                    [pick(yb, yb_in, j, part) for j in (-2, -1, 0, 1, 2)],
                    *[
                        [pick(h, o, j, part) for j in (-1, 0, 1)]
                        for h, o in ((yd, yd_in), (zd, zd_in), (yi, yi_in))
                    ],
                )
                for n, value in enumerate(values):
                    obuf[n, 2 * side + s, part] = value.astype(jnp.bfloat16)
            finish(2 * side + s).start()
    for k in range(4):
        finish(k).wait()
    late.wait()


def cost(us):
    return pl.CostEstimate(flops=int(us * 4e6), bytes_accessed=int(us * 1e6), transcendentals=0)


def shape(*dims, dtype=F32):
    return jax.ShapeDtypeStruct(dims, dtype)


def local(material, eps_table, grading):
    nx, ny, nz = material.shape
    rows = ny + 8
    material, eps_table, grading = (
        pltpu.with_memory_space_constraint(a, pltpu.HBM) for a in (material, eps_table, grading)
    )
    forward = [(i, (i + 1) % 8) for i in range(8)]
    backward = [(b, a) for a, b in forward]
    pairs = [[0, 1], [2, 3], [4, 5], [6, 7]]
    odd = [((i + 1) % 8, ((i ^ 1) + 1) % 8) for i in range(8)]
    parity = (lax.axis_index("gz") & 1).reshape(1)
    vmem = pltpu.CompilerParams(vmem_limit_bytes=24 << 20)

    y_face = shape(2 * nx + 8, nz)
    y_fwd, y_bwd, mat_near, gra_near, table_rows = pl.pallas_call(
        face_kernel,
        in_specs=[HBM] * 3,
        out_specs=[VMEM] * 5,
        out_shape=[
            y_face,
            y_face,
            shape(nx, ny, nz, dtype=jnp.int32),
            shape(nx, ny, nz, dtype=jnp.bfloat16),
            shape(8, nz),
        ],
        scratch_shapes=[
            pltpu.SMEM((8,), F32),
            pltpu.SemaphoreType.DMA((3, nx // STEP)),
        ],
        compiler_params=vmem,
        cost_estimate=cost(1),
        name="face",
    )(eps_table, material, grading)
    y_low = lax.ppermute(y_fwd, "gy", forward)
    y_high = lax.ppermute(y_bwd, "gy", backward)

    eps, packed = pl.pallas_call(
        block_kernel,
        in_specs=[VMEM] * 3,
        out_specs=[VMEM] * 2,
        out_shape=[shape(nx, ny, nz), shape(ny, nz)],
        compiler_params=vmem,
        cost_estimate=cost(3),
        name="block",
    )(table_rows, mat_near, gra_near)

    z_face = pl.pallas_call(
        zface_kernel,
        in_specs=[VMEM] * 3,
        out_specs=VMEM,
        out_shape=shape(rows, nz),
        compiler_params=vmem,
        cost_estimate=cost(0.2),
        name="zface",
    )(packed, y_low, y_high)
    z_odd = lax.ppermute(z_face, "gz", odd)
    z_even = lax.all_gather(z_face, "gz", axis=0, axis_index_groups=pairs)

    x_fwd, x_bwd = pl.pallas_call(
        xface_kernel,
        in_specs=[SMEM] + [VMEM] * 5,
        out_specs=[VMEM, VMEM],
        out_shape=[shape(2 * rows + 8, nz)] * 2,
        compiler_params=vmem,
        cost_estimate=cost(0.5),
        name="xface",
    )(parity, eps, y_low, y_high, z_even, z_odd)
    x_low = lax.ppermute(x_fwd, "gx", forward)
    x_high = lax.ppermute(x_bwd, "gx", backward)

    full = (nx, ny + 16, nz)
    late = nx - 4 - EARLY * GROUP
    out, *edges = pl.pallas_call(
        inner_kernel,
        in_specs=[SMEM] + [VMEM] * 5,
        out_specs=[ANY] + [VMEM] * 5,
        out_shape=[shape(6, nx, ny, nz, dtype=jnp.bfloat16)]
        + [shape(nx, ny, nz)] * 4
        + [shape(6, late, ny, nz, dtype=jnp.bfloat16)],
        scratch_shapes=[
            pltpu.VMEM((nx, 8, nz), F32),
            pltpu.VMEM((rows, nz), F32),
            pltpu.VMEM((nx, rows, nz), F32),
            pltpu.VMEM((512, 256), jnp.bfloat16),
            *[pltpu.VMEM((nx, ny + 16, nz), F32)] * 3,
            pltpu.VMEM((6, nx - 4 - late, ny, nz), jnp.bfloat16),
            pltpu.SemaphoreType.DMA(((nx - 4 - late) // GROUP,)),
        ],
        compiler_params=vmem,
        cost_estimate=cost(6),
        name="inner",
    )(parity, eps, y_low, y_high, z_even, z_odd)

    return pl.pallas_call(
        outer_kernel,
        in_specs=[VMEM] * 7 + [ANY],
        out_specs=ANY,
        out_shape=shape(6, nx, ny, nz, dtype=jnp.bfloat16),
        input_output_aliases={7: 0},
        scratch_shapes=[
            *[pltpu.VMEM((4, ny + 16, nz), F32)] * 3,
            *[pltpu.VMEM((4, ny, nz), F32)] * 4,
            pltpu.VMEM((6, 4, ny, nz), jnp.bfloat16),
            pltpu.SemaphoreType.DMA((5,)),
        ],
        compiler_params=vmem,
        cost_estimate=cost(1),
        name="outer",
    )(x_low, x_high, *edges, out)


def solution(mesh):
    return jax.shard_map(
        local,
        mesh=mesh,
        in_specs=(P("gx", "gy", "gz"), P(), P("gx", "gy", "gz")),
        out_specs=P(None, "gx", "gy", "gz"),
        check_vma=False,
    )
```

```python
import jax
import jax.numpy as jnp
from jax import lax
from jax.experimental import pallas as pl
from jax.experimental.pallas import tpu as pltpu
from jax.sharding import PartitionSpec as P

F32 = jnp.float32
VMEM = pl.BlockSpec(memory_space=pltpu.VMEM)
SMEM = pl.BlockSpec(memory_space=pltpu.SMEM)
ANY = pl.BlockSpec(memory_space=pl.ANY)
HBM = pl.BlockSpec(memory_space=pltpu.HBM)


def lookup(material, table, grading):
    low = (material & 1) != 0
    mid = (material & 2) != 0
    top = (material & 4) != 0
    pair = [jnp.where(low, table[2 * k + 1], table[2 * k]) for k in range(4)]
    quad = [jnp.where(mid, pair[2 * k + 1], pair[2 * k]) for k in range(2)]
    return jnp.where(top, quad[1], quad[0]) * grading.astype(F32)


def lanes(shape):
    return lax.broadcasted_iota(jnp.int32, shape, len(shape) - 1)


def scalars(table_ref):
    return [table_ref[k] for k in range(8)]


def finish_face(ref, rows, nx):
    ref[2 * nx : 2 * nx + 2] = rows
    ref[2 * nx + 2 : 2 * nx + 8] = jnp.ones((6, 128), F32)


def face_kernel(
    table_hbm, mat_hbm, gra_hbm, fwd_ref, bwd_ref, mat_ref, gra_ref, rows_ref, table_ref, sem
):
    nx, ny = mat_hbm.shape[0], mat_hbm.shape[1]
    begin = pltpu.make_async_copy(table_hbm, table_ref, sem.at[2, 0])
    begin.start()
    copies = []
    for c in range(nx // STEP):
        part = slice(c * STEP, (c + 1) * STEP)
        copies.append(
            [
                pltpu.make_async_copy(src.at[part], dst.at[part], sem.at[k, c])
                for k, (src, dst) in enumerate(((mat_hbm, mat_ref), (gra_hbm, gra_ref)))
            ]
        )
        for copy in copies[c]:
            copy.start()
    begin.wait()
    table = scalars(table_ref)
    for k in range(8):
        rows_ref[k : k + 1] = jnp.full((1, 128), table[k], F32)
    lane = lanes((8, 128))
    packed = [jnp.zeros((8, 128), F32)] * 2
    for x in range(nx):
        if x % STEP == 0:
            for copy in copies[x // STEP]:
                copy.wait()
        low = lookup(mat_ref[x, 0:8], table, gra_ref[x, 0:8])
        high = lookup(mat_ref[x, ny - 8 : ny], table, gra_ref[x, ny - 8 : ny])
        bwd_ref[2 * x : 2 * x + 2] = low[0:2]
        fwd_ref[2 * x : 2 * x + 2] = high[6:8]
        turn = (4 * x + 2) % 128
        packed = [
            jnp.where((lane >> 2) == x, pltpu.roll(v, turn, 1) if turn else v, p)
            for v, p in zip((low, high), packed)
        ]
    finish_face(bwd_ref, packed[0][0:2], nx)
    finish_face(fwd_ref, packed[1][6:8], nx)


STEP = 8


def block_kernel(rows_ref, mat_ref, gra_ref, eps_ref, packed_ref):
    nx, ny = mat_ref.shape[0], mat_ref.shape[1]
    table = [jnp.broadcast_to(rows_ref[k : k + 1], (ny, 128)) for k in range(8)]
    lane = lanes((ny, 128))

    def one(c, packed):
        for k in range(STEP):
            x = c * STEP + k
            value = lookup(mat_ref[x], table, gra_ref[x])
            eps_ref[x] = value
            packed = jnp.where(
                (lane >> 2) == x, pltpu.roll(value, lax.rem(4 * x + 2, 128), 1), packed
            )
        return packed

    packed_ref[...] = lax.fori_loop(0, nx // STEP, one, jnp.zeros((ny, 128), F32))


def zface_kernel(packed_ref, low_ref, high_ref, out_ref):
    ny = packed_ref.shape[0]
    out_ref[0:ny] = packed_ref[...]
    out_ref[ny : ny + 2] = low_ref[64:66]
    out_ref[ny + 2 : ny + 4] = high_ref[64:66]
    out_ref[ny + 4 : ny + 8] = jnp.ones((4, 128), F32)


def joined(parity_ref, even_ref, odd_ref):
    lane = lanes(odd_ref.shape)
    parity = parity_ref[0]
    return jnp.where(((lane >> 1) & 1) == parity, odd_ref[...], even_ref[1 - parity])


def xface_kernel(parity_ref, eps_ref, low_ref, high_ref, even_ref, odd_ref, fwd_ref, bwd_ref):
    nx, ny = eps_ref.shape[0], eps_ref.shape[1]
    rows = ny + 8
    halo = joined(parity_ref, even_ref, odd_ref)
    lane = lanes((8, 128))
    for ref, start in ((fwd_ref, nx - 2), (bwd_ref, 0)):
        for s in range(2):
            x = start + s
            ref[s * rows : s * rows + ny] = eps_ref[x]
            ref[s * rows + ny : s * rows + ny + 2] = low_ref[2 * x : 2 * x + 2]
            ref[s * rows + ny + 2 : s * rows + ny + 4] = high_ref[2 * x : 2 * x + 2]
            ref[s * rows + ny + 4 : s * rows + rows] = jnp.ones((4, 128), F32)
        packed = jnp.ones((8, 128), F32)
        for g in range(rows // 8):
            turn = (8 * g - 4 * start) % 128
            part = halo[8 * g : 8 * g + 8]
            packed = jnp.where((lane >> 3) == g, pltpu.roll(part, turn, 1) if turn else part, packed)
        ref[2 * rows : 2 * rows + 8] = packed


def zsums(v, h, lane):
    left = pltpu.roll(jnp.where(lane == 127, h, v), 1, 1)
    left2 = pltpu.roll(jnp.where(lane >= 126, h, v), 2, 1)
    right = pltpu.roll(jnp.where(lane == 0, h, v), 127, 1)
    right2 = pltpu.roll(jnp.where(lane <= 1, h, v), 126, 1)
    inv, inv_h = 1.0 / v, 1.0 / h
    inv_left = pltpu.roll(jnp.where(lane == 127, inv_h, inv), 1, 1)
    inv_right = pltpu.roll(jnp.where(lane == 0, inv_h, inv), 127, 1)
    return v + left + right, (right + right2) - (left + left2), inv + inv_left + inv_right


def inverse_zsum(v, h, lane):
    inv, inv_h = 1.0 / v, 1.0 / h
    inv_left = pltpu.roll(jnp.where(lane == 127, inv_h, inv), 1, 1)
    inv_right = pltpu.roll(jnp.where(lane == 0, inv_h, inv), 127, 1)
    return inv + inv_left + inv_right


def tap_matrix():
    shape = (512, 256)
    row = lax.broadcasted_iota(jnp.int32, shape, 0) & 255
    column = lax.broadcasted_iota(jnp.int32, shape, 1)
    place = jnp.where(row < 128, row, jnp.where(row >= 192, row - 256, row))
    away = place - (column & 127)
    box = jnp.where(jnp.abs(away) <= 1, 1.0, 0.0)
    outer = jnp.where((jnp.abs(away) == 1) | (jnp.abs(away) == 2), 1.0, 0.0)
    der = jnp.where(away > 0, outer, -outer)
    return jnp.where(column < 128, box, der).astype(jnp.bfloat16)


def put(ref, index, value, ny):
    ref[index, 8 : 8 + ny] = value[0:ny]
    ref[index, 6:8] = value[ny : ny + 2]
    ref[index, 8 + ny : 10 + ny] = value[ny + 2 : ny + 4]


def ysums(refs, index, count, r):
    box, der, inv = refs
    b = [box[index, 8 + r + k : 8 + r + k + count] for k in (-2, -1, 0, 1, 2)]
    d = [der[index, 8 + r + k : 8 + r + k + count] for k in (-1, 0, 1)]
    i = [inv[index, 8 + r + k : 8 + r + k + count] for k in (-1, 0, 1)]
    return (
        b[1] + b[2] + b[3],
        (b[4] + b[3]) - (b[1] + b[0]),
        d[0] + d[1] + d[2],
        i[0] + i[1] + i[2],
    )


def result(yb, yd, zd, yi):
    mean = yb[1] + yb[2] + yb[3]
    gx = (yb[4] + yb[3]) - (yb[1] + yb[0])
    gy = yd[0] + yd[1] + yd[2]
    gz = zd[0] + zd[1] + zd[2]
    inv = yi[0] + yi[1] + yi[2]
    recip = 27.0 / mean
    factor = (inv * (1.0 / 27.0) - recip) / (gx * gx + gy * gy + gz * gz + 291.6)
    fx, fy, fz = gx * factor, gy * factor, gz * factor
    return (gx * fx + recip, gy * fy + recip, gz * fz + recip, gx * fy, gx * fz, gy * fz)


GROUP = 4
BEHIND = 3 + 4 // GROUP
EARLY = 4


def inner_kernel(
    parity_ref, eps_ref, low_ref, high_ref, even_ref, odd_ref,
    out_ref, yb, yd, zd, yi, tail,
    rim, halo, side, taps, box, der, inv, obuf, sem,
):
    nx, ny = eps_ref.shape[0], eps_ref.shape[1]
    halo[...] = joined(parity_ref, even_ref, odd_ref)
    taps[...] = tap_matrix()
    lane = lanes((8, 128))
    ones = jnp.ones((4, 128), F32)
    for x in range(nx):
        rim[x, 0:2] = low_ref[2 * x : 2 * x + 2]
        rim[x, 2:4] = high_ref[2 * x : 2 * x + 2]
        rim[x, 4:8] = ones

    def turned(x):
        for r in range(0, ny + 8, 8):
            side[x, r : r + 8] = pltpu.roll(halo[r : r + 8], lax.rem(254 - 4 * x, 128), 1)

    def along_z(c):
        slices = range(GROUP)
        for k in slices:
            x = c * GROUP + k
            for r in range(0, ny, 8):
                value = inverse_zsum(eps_ref[x, r : r + 8], side[x, r : r + 8], lane)
                inv[x, 8 + r : 16 + r] = value
            value = inverse_zsum(rim[x], side[x, ny : ny + 8], lane)
            inv[x, 6:8] = value[0:2]
            inv[x, 8 + ny : 10 + ny] = value[2:4]
        own = jnp.concatenate(
            [part for k in slices for part in (eps_ref[c * GROUP + k], rim[c * GROUP + k])], axis=0
        )
        near = jnp.concatenate([side[c * GROUP + k] for k in slices], axis=0)
        values = jnp.concatenate([own, near], axis=1)
        coarse = values.astype(jnp.bfloat16)
        fine = (values - coarse.astype(F32)).astype(jnp.bfloat16)
        sums = jnp.dot(
            jnp.concatenate([coarse, fine], axis=1), taps[...], preferred_element_type=F32
        )
        for ref, part in ((box, sums[:, 0:128]), (der, sums[:, 128:256])):
            for k in slices:
                x, at = c * GROUP + k, k * (ny + 8)
                ref[x, 8 : 8 + ny] = part[at : at + ny]
                ref[x, 6:8] = part[at + ny : at + ny + 2]
                ref[x, 8 + ny : 10 + ny] = part[at + ny + 2 : at + ny + 4]

    def along_y(x):
        for r in range(0, ny, 8):
            for ref, value in zip((yb, yd, zd, yi), ysums((box, der, inv), x, 8, r)):
                ref[x, r : r + 8] = value

    def along_x(x, buffer, at):
        for r in range(0, ny, 16):
            part = slice(r, r + 16)
            values = result(
                [yb[x + j, part] for j in (-2, -1, 0, 1, 2)],
                *[[ref[x + j, part] for j in (-1, 0, 1)] for ref in (yd, zd, yi)],
            )
            for n, value in enumerate(values):
                buffer[n, at, part] = value.astype(jnp.bfloat16)

    def copy(c):
        part = GROUP * c
        return pltpu.make_async_copy(
            obuf.at[:, pl.ds(part, GROUP)], out_ref.at[:, pl.ds(2 + part, GROUP)], sem.at[c]
        )

    groups = nx // GROUP
    last = (nx - 4) // GROUP
    early = EARLY
    stages = (
        (turned, 0, groups),
        (along_z, 1, groups),
        (along_y, 2, groups),
        (along_x, BEHIND, last),
    )

    def run(j, active, soon):
        for stage, lag in active:
            if stage is along_z:
                stage(j - lag)
                continue
            for k in range(GROUP):
                x = (j - lag) * GROUP + k
                if stage is not along_x:
                    stage(x)
                elif soon:
                    stage(x + 2, obuf, x)
                else:
                    stage(x + 2, tail, x - early * GROUP)
        if active[0][0] is along_x and soon:
            copy(j - BEHIND).start()

    edges = sorted(
        {lag for _, lag, _ in stages} | {lag + n for _, lag, n in stages} | {BEHIND + early}
    )
    for start, stop in zip(edges, edges[1:]):
        active = [(stage, lag) for stage, lag, n in stages[::-1] if lag <= start < lag + n]

        def body(j, carry, active=active, soon=start < BEHIND + early):
            run(j, active, soon)
            return carry

        if active:
            lax.fori_loop(start, stop, body, 0)

    def finish(c, carry):
        copy(c).wait()
        return carry

    lax.fori_loop(0, early, finish, 0)


def outer_kernel(
    low_ref, high_ref, yb_in, yd_in, zd_in, yi_in, tail, _, out_ref,
    box, der, inv, yb, yd, zd, yi, obuf, sem,
):
    nx, ny = out_ref.shape[1], out_ref.shape[2]
    rows = ny + 8
    late = pltpu.make_async_copy(
        tail, out_ref.at[:, pl.ds(nx - 2 - tail.shape[1], tail.shape[1])], sem.at[4]
    )
    late.start()

    def finish(k):
        x = k if k < 2 else nx - 4 + k
        return pltpu.make_async_copy(
            obuf.at[:, pl.ds(k, 1)], out_ref.at[:, pl.ds(x, 1)], sem.at[k]
        )

    lane = lanes((rows, 128))
    for k, (ref, s) in enumerate(((low_ref, 0), (low_ref, 1), (high_ref, 0), (high_ref, 1))):
        v = ref[s * rows : (s + 1) * rows]
        packed = ref[2 * rows : 2 * rows + 8]
        h = jnp.concatenate(
            [pltpu.roll(packed, (126 - 8 * g - 4 * s) % 128, 1) for g in range(rows // 8)], axis=0
        )
        for dst, value in zip((box, der, inv), zsums(v, h, lane)):
            put(dst, k, value, ny)
    for k in range(4):
        for r in range(0, ny, 16):
            for ref, value in zip((yb, yd, zd, yi), ysums((box, der, inv), k, 16, r)):
                ref[k, r : r + 16] = value
    for side in range(2):
        for s in range(2):
            def pick(halo_ref, own_ref, j, part):
                x = s + j
                if side == 0:
                    return halo_ref[2 + x, part] if x < 0 else own_ref[x, part]
                x = x - 2
                return halo_ref[2 + x, part] if x >= 0 else own_ref[nx + x, part]

            for r in range(0, ny, 16):
                part = slice(r, r + 16)
                values = result(
                    [pick(yb, yb_in, j, part) for j in (-2, -1, 0, 1, 2)],
                    *[
                        [pick(h, o, j, part) for j in (-1, 0, 1)]
                        for h, o in ((yd, yd_in), (zd, zd_in), (yi, yi_in))
                    ],
                )
                for n, value in enumerate(values):
                    obuf[n, 2 * side + s, part] = value.astype(jnp.bfloat16)
            finish(2 * side + s).start()
    for k in range(4):
        finish(k).wait()
    late.wait()


def cost(us):
    return pl.CostEstimate(flops=int(us * 4e6), bytes_accessed=int(us * 1e6), transcendentals=0)


def shape(*dims, dtype=F32):
    return jax.ShapeDtypeStruct(dims, dtype)


def local(material, eps_table, grading):
    nx, ny, nz = material.shape
    rows = ny + 8
    material, eps_table, grading = (
        pltpu.with_memory_space_constraint(a, pltpu.HBM) for a in (material, eps_table, grading)
    )
    forward = [(i, (i + 1) % 8) for i in range(8)]
    backward = [(b, a) for a, b in forward]
    pairs = [[0, 1], [2, 3], [4, 5], [6, 7]]
    odd = [((i + 1) % 8, ((i ^ 1) + 1) % 8) for i in range(8)]
    parity = (lax.axis_index("gz") & 1).reshape(1)
    vmem = pltpu.CompilerParams(vmem_limit_bytes=24 << 20)

    y_face = shape(2 * nx + 8, nz)
    y_fwd, y_bwd, mat_near, gra_near, table_rows = pl.pallas_call(
        face_kernel,
        in_specs=[HBM] * 3,
        out_specs=[VMEM] * 5,
        out_shape=[
            y_face,
            y_face,
            shape(nx, ny, nz, dtype=jnp.int32),
            shape(nx, ny, nz, dtype=jnp.bfloat16),
            shape(8, nz),
        ],
        scratch_shapes=[
            pltpu.SMEM((8,), F32),
            pltpu.SemaphoreType.DMA((3, nx // STEP)),
        ],
        compiler_params=vmem,
        cost_estimate=cost(1),
        name="face",
    )(eps_table, material, grading)
    y_low = lax.ppermute(y_fwd, "gy", forward)
    y_high = lax.ppermute(y_bwd, "gy", backward)

    eps, packed = pl.pallas_call(
        block_kernel,
        in_specs=[VMEM] * 3,
        out_specs=[VMEM] * 2,
        out_shape=[shape(nx, ny, nz), shape(ny, nz)],
        compiler_params=vmem,
        cost_estimate=cost(3),
        name="block",
    )(table_rows, mat_near, gra_near)

    z_face = pl.pallas_call(
        zface_kernel,
        in_specs=[VMEM] * 3,
        out_specs=VMEM,
        out_shape=shape(rows, nz),
        compiler_params=vmem,
        cost_estimate=cost(0.2),
        name="zface",
    )(packed, y_low, y_high)
    z_odd = lax.ppermute(z_face, "gz", odd)
    z_even = lax.all_gather(z_face, "gz", axis=0, axis_index_groups=pairs)

    x_fwd, x_bwd = pl.pallas_call(
        xface_kernel,
        in_specs=[SMEM] + [VMEM] * 5,
        out_specs=[VMEM, VMEM],
        out_shape=[shape(2 * rows + 8, nz)] * 2,
        compiler_params=vmem,
        cost_estimate=cost(0.5),
        name="xface",
    )(parity, eps, y_low, y_high, z_even, z_odd)
    x_low = lax.ppermute(x_fwd, "gx", forward)
    x_high = lax.ppermute(x_bwd, "gx", backward)

    full = (nx, ny + 16, nz)
    late = nx - 4 - EARLY * GROUP
    out, *edges = pl.pallas_call(
        inner_kernel,
        in_specs=[SMEM] + [VMEM] * 5,
        out_specs=[ANY] + [VMEM] * 5,
        out_shape=[shape(6, nx, ny, nz, dtype=jnp.bfloat16)]
        + [shape(nx, ny, nz)] * 4
        + [shape(6, late, ny, nz, dtype=jnp.bfloat16)],
        scratch_shapes=[
            pltpu.VMEM((nx, 8, nz), F32),
            pltpu.VMEM((rows, nz), F32),
            pltpu.VMEM((nx, rows, nz), F32),
            pltpu.VMEM((512, 256), jnp.bfloat16),
            *[pltpu.VMEM((nx, ny + 16, nz), F32)] * 3,
            pltpu.VMEM((6, nx - 4 - late, ny, nz), jnp.bfloat16),
            pltpu.SemaphoreType.DMA(((nx - 4 - late) // GROUP,)),
        ],
        compiler_params=vmem,
        cost_estimate=cost(6),
        name="inner",
    )(parity, eps, y_low, y_high, z_even, z_odd)

    return pl.pallas_call(
        outer_kernel,
        in_specs=[VMEM] * 7 + [ANY],
        out_specs=ANY,
        out_shape=shape(6, nx, ny, nz, dtype=jnp.bfloat16),
        input_output_aliases={7: 0},
        scratch_shapes=[
            *[pltpu.VMEM((4, ny + 16, nz), F32)] * 3,
            *[pltpu.VMEM((4, ny, nz), F32)] * 4,
            pltpu.VMEM((6, 4, ny, nz), jnp.bfloat16),
            pltpu.SemaphoreType.DMA((5,)),
        ],
        compiler_params=vmem,
        cost_estimate=cost(1),
        name="outer",
    )(x_low, x_high, *edges, out)


def solution(mesh):
    return jax.shard_map(
        local,
        mesh=mesh,
        in_specs=(P("gx", "gy", "gz"), P(), P("gx", "gy", "gz")),
        out_specs=P(None, "gx", "gy", "gz"),
        check_vma=False,
    )
```

```python
import jax
import jax.numpy as jnp
from jax import lax
from jax.experimental import pallas as pl
from jax.experimental.pallas import tpu as pltpu
from jax.sharding import PartitionSpec as P

F32 = jnp.float32
VMEM = pl.BlockSpec(memory_space=pltpu.VMEM)
SMEM = pl.BlockSpec(memory_space=pltpu.SMEM)
ANY = pl.BlockSpec(memory_space=pl.ANY)
HBM = pl.BlockSpec(memory_space=pltpu.HBM)


def lookup(material, table, grading):
    low = (material & 1) != 0
    mid = (material & 2) != 0
    top = (material & 4) != 0
    pair = [jnp.where(low, table[2 * k + 1], table[2 * k]) for k in range(4)]
    quad = [jnp.where(mid, pair[2 * k + 1], pair[2 * k]) for k in range(2)]
    return jnp.where(top, quad[1], quad[0]) * grading.astype(F32)


def lanes(shape):
    return lax.broadcasted_iota(jnp.int32, shape, len(shape) - 1)


def scalars(table_ref):
    return [table_ref[k] for k in range(8)]


def finish_face(ref, rows, nx):
    ref[2 * nx : 2 * nx + 2] = rows
    ref[2 * nx + 2 : 2 * nx + 8] = jnp.ones((6, 128), F32)


def face_kernel(
    table_hbm, mat_hbm, gra_hbm, fwd_ref, bwd_ref, mat_ref, gra_ref, rows_ref, table_ref, sem
):
    nx, ny = mat_hbm.shape[0], mat_hbm.shape[1]
    begin = pltpu.make_async_copy(table_hbm, table_ref, sem.at[2, 0])
    begin.start()
    copies = []
    for c in range(nx // STEP):
        part = slice(c * STEP, (c + 1) * STEP)
        copies.append(
            [
                pltpu.make_async_copy(src.at[part], dst.at[part], sem.at[k, c])
                for k, (src, dst) in enumerate(((mat_hbm, mat_ref), (gra_hbm, gra_ref)))
            ]
        )
        for copy in copies[c]:
            copy.start()
    begin.wait()
    table = scalars(table_ref)
    for k in range(8):
        rows_ref[k : k + 1] = jnp.full((1, 128), table[k], F32)
    lane = lanes((8, 128))
    packed = [jnp.zeros((8, 128), F32)] * 2
    for x in range(nx):
        if x % STEP == 0:
            for copy in copies[x // STEP]:
                copy.wait()
        low = lookup(mat_ref[x, 0:8], table, gra_ref[x, 0:8])
        high = lookup(mat_ref[x, ny - 8 : ny], table, gra_ref[x, ny - 8 : ny])
        bwd_ref[2 * x : 2 * x + 2] = low[0:2]
        fwd_ref[2 * x : 2 * x + 2] = high[6:8]
        turn = (4 * x + 2) % 128
        packed = [
            jnp.where((lane >> 2) == x, pltpu.roll(v, turn, 1) if turn else v, p)
            for v, p in zip((low, high), packed)
        ]
    finish_face(bwd_ref, packed[0][0:2], nx)
    finish_face(fwd_ref, packed[1][6:8], nx)


STEP = 4


def block_kernel(rows_ref, mat_ref, gra_ref, eps_ref, packed_ref):
    nx, ny = mat_ref.shape[0], mat_ref.shape[1]
    table = [jnp.broadcast_to(rows_ref[k : k + 1], (ny, 128)) for k in range(8)]
    lane = lanes((ny, 128))

    def one(c, packed):
        for k in range(STEP):
            x = c * STEP + k
            value = lookup(mat_ref[x], table, gra_ref[x])
            eps_ref[x] = value
            packed = jnp.where(
                (lane >> 2) == x, pltpu.roll(value, lax.rem(4 * x + 2, 128), 1), packed
            )
        return packed

    packed_ref[...] = lax.fori_loop(0, nx // STEP, one, jnp.zeros((ny, 128), F32))


def zface_kernel(packed_ref, low_ref, high_ref, out_ref):
    ny = packed_ref.shape[0]
    out_ref[0:ny] = packed_ref[...]
    out_ref[ny : ny + 2] = low_ref[64:66]
    out_ref[ny + 2 : ny + 4] = high_ref[64:66]
    out_ref[ny + 4 : ny + 8] = jnp.ones((4, 128), F32)


def joined(parity_ref, even_ref, odd_ref):
    lane = lanes(odd_ref.shape)
    parity = parity_ref[0]
    return jnp.where(((lane >> 1) & 1) == parity, odd_ref[...], even_ref[1 - parity])


def xface_kernel(parity_ref, eps_ref, low_ref, high_ref, even_ref, odd_ref, fwd_ref, bwd_ref):
    nx, ny = eps_ref.shape[0], eps_ref.shape[1]
    rows = ny + 8
    halo = joined(parity_ref, even_ref, odd_ref)
    lane = lanes((8, 128))
    for ref, start in ((fwd_ref, nx - 2), (bwd_ref, 0)):
        for s in range(2):
            x = start + s
            ref[s * rows : s * rows + ny] = eps_ref[x]
            ref[s * rows + ny : s * rows + ny + 2] = low_ref[2 * x : 2 * x + 2]
            ref[s * rows + ny + 2 : s * rows + ny + 4] = high_ref[2 * x : 2 * x + 2]
            ref[s * rows + ny + 4 : s * rows + rows] = jnp.ones((4, 128), F32)
        packed = jnp.ones((8, 128), F32)
        for g in range(rows // 8):
            turn = (8 * g - 4 * start) % 128
            part = halo[8 * g : 8 * g + 8]
            packed = jnp.where((lane >> 3) == g, pltpu.roll(part, turn, 1) if turn else part, packed)
        ref[2 * rows : 2 * rows + 8] = packed


def zsums(v, h, lane):
    left = pltpu.roll(jnp.where(lane == 127, h, v), 1, 1)
    left2 = pltpu.roll(jnp.where(lane >= 126, h, v), 2, 1)
    right = pltpu.roll(jnp.where(lane == 0, h, v), 127, 1)
    right2 = pltpu.roll(jnp.where(lane <= 1, h, v), 126, 1)
    inv, inv_h = 1.0 / v, 1.0 / h
    inv_left = pltpu.roll(jnp.where(lane == 127, inv_h, inv), 1, 1)
    inv_right = pltpu.roll(jnp.where(lane == 0, inv_h, inv), 127, 1)
    return v + left + right, (right + right2) - (left + left2), inv + inv_left + inv_right


def inverse_zsum(v, h, lane):
    inv, inv_h = 1.0 / v, 1.0 / h
    inv_left = pltpu.roll(jnp.where(lane == 127, inv_h, inv), 1, 1)
    inv_right = pltpu.roll(jnp.where(lane == 0, inv_h, inv), 127, 1)
    return inv + inv_left + inv_right


def tap_matrix():
    shape = (512, 256)
    row = lax.broadcasted_iota(jnp.int32, shape, 0) & 255
    column = lax.broadcasted_iota(jnp.int32, shape, 1)
    place = jnp.where(row < 128, row, jnp.where(row >= 192, row - 256, row))
    away = place - (column & 127)
    box = jnp.where(jnp.abs(away) <= 1, 1.0, 0.0)
    outer = jnp.where((jnp.abs(away) == 1) | (jnp.abs(away) == 2), 1.0, 0.0)
    der = jnp.where(away > 0, outer, -outer)
    return jnp.where(column < 128, box, der).astype(jnp.bfloat16)


def put(ref, index, value, ny):
    ref[index, 8 : 8 + ny] = value[0:ny]
    ref[index, 6:8] = value[ny : ny + 2]
    ref[index, 8 + ny : 10 + ny] = value[ny + 2 : ny + 4]


def ysums(refs, index, count, r):
    box, der, inv = refs
    b = [box[index, 8 + r + k : 8 + r + k + count] for k in (-2, -1, 0, 1, 2)]
    d = [der[index, 8 + r + k : 8 + r + k + count] for k in (-1, 0, 1)]
    i = [inv[index, 8 + r + k : 8 + r + k + count] for k in (-1, 0, 1)]
    return (
        b[1] + b[2] + b[3],
        (b[4] + b[3]) - (b[1] + b[0]),
        d[0] + d[1] + d[2],
        i[0] + i[1] + i[2],
    )


def result(yb, yd, zd, yi):
    mean = yb[1] + yb[2] + yb[3]
    gx = (yb[4] + yb[3]) - (yb[1] + yb[0])
    gy = yd[0] + yd[1] + yd[2]
    gz = zd[0] + zd[1] + zd[2]
    inv = yi[0] + yi[1] + yi[2]
    recip = 27.0 / mean
    factor = (inv * (1.0 / 27.0) - recip) / (gx * gx + gy * gy + gz * gz + 291.6)
    fx, fy, fz = gx * factor, gy * factor, gz * factor
    return (gx * fx + recip, gy * fy + recip, gz * fz + recip, gx * fy, gx * fz, gy * fz)


GROUP = 4
BEHIND = 3 + 4 // GROUP
EARLY = 3


def inner_kernel(
    parity_ref, eps_ref, low_ref, high_ref, even_ref, odd_ref,
    out_ref, yb, yd, zd, yi, tail,
    rim, halo, side, taps, box, der, inv, obuf, sem,
):
    nx, ny = eps_ref.shape[0], eps_ref.shape[1]
    halo[...] = joined(parity_ref, even_ref, odd_ref)
    taps[...] = tap_matrix()
    lane = lanes((8, 128))
    ones = jnp.ones((4, 128), F32)
    for x in range(nx):
        rim[x, 0:2] = low_ref[2 * x : 2 * x + 2]
        rim[x, 2:4] = high_ref[2 * x : 2 * x + 2]
        rim[x, 4:8] = ones

    def turned(x):
        for r in range(0, ny + 8, 8):
            side[x, r : r + 8] = pltpu.roll(halo[r : r + 8], lax.rem(254 - 4 * x, 128), 1)

    def along_z(c):
        slices = range(GROUP)
        for k in slices:
            x = c * GROUP + k
            for r in range(0, ny, 8):
                value = inverse_zsum(eps_ref[x, r : r + 8], side[x, r : r + 8], lane)
                inv[x, 8 + r : 16 + r] = value
            value = inverse_zsum(rim[x], side[x, ny : ny + 8], lane)
            inv[x, 6:8] = value[0:2]
            inv[x, 8 + ny : 10 + ny] = value[2:4]
        own = jnp.concatenate(
            [part for k in slices for part in (eps_ref[c * GROUP + k], rim[c * GROUP + k])], axis=0
        )
        near = jnp.concatenate([side[c * GROUP + k] for k in slices], axis=0)
        values = jnp.concatenate([own, near], axis=1)
        coarse = values.astype(jnp.bfloat16)
        fine = (values - coarse.astype(F32)).astype(jnp.bfloat16)
        sums = jnp.dot(
            jnp.concatenate([coarse, fine], axis=1), taps[...], preferred_element_type=F32
        )
        for ref, part in ((box, sums[:, 0:128]), (der, sums[:, 128:256])):
            for k in slices:
                x, at = c * GROUP + k, k * (ny + 8)
                ref[x, 8 : 8 + ny] = part[at : at + ny]
                ref[x, 6:8] = part[at + ny : at + ny + 2]
                ref[x, 8 + ny : 10 + ny] = part[at + ny + 2 : at + ny + 4]

    def along_y(x):
        for r in range(0, ny, 8):
            for ref, value in zip((yb, yd, zd, yi), ysums((box, der, inv), x, 8, r)):
                ref[x, r : r + 8] = value

    def along_x(x, buffer, at):
        for r in range(0, ny, 16):
            part = slice(r, r + 16)
            values = result(
                [yb[x + j, part] for j in (-2, -1, 0, 1, 2)],
                *[[ref[x + j, part] for j in (-1, 0, 1)] for ref in (yd, zd, yi)],
            )
            for n, value in enumerate(values):
                buffer[n, at, part] = value.astype(jnp.bfloat16)

    def copy(c):
        part = GROUP * c
        return pltpu.make_async_copy(
            obuf.at[:, pl.ds(part, GROUP)], out_ref.at[:, pl.ds(2 + part, GROUP)], sem.at[c]
        )

    groups = nx // GROUP
    last = (nx - 4) // GROUP
    early = EARLY
    stages = (
        (turned, 0, groups),
        (along_z, 1, groups),
        (along_y, 2, groups),
        (along_x, BEHIND, last),
    )

    def run(j, active, soon):
        for stage, lag in active:
            if stage is along_z:
                stage(j - lag)
                continue
            for k in range(GROUP):
                x = (j - lag) * GROUP + k
                if stage is not along_x:
                    stage(x)
                elif soon:
                    stage(x + 2, obuf, x)
                else:
                    stage(x + 2, tail, x - early * GROUP)
        if active[0][0] is along_x and soon:
            copy(j - BEHIND).start()

    edges = sorted(
        {lag for _, lag, _ in stages} | {lag + n for _, lag, n in stages} | {BEHIND + early}
    )
    for start, stop in zip(edges, edges[1:]):
        active = [(stage, lag) for stage, lag, n in stages[::-1] if lag <= start < lag + n]

        def body(j, carry, active=active, soon=start < BEHIND + early):
            run(j, active, soon)
            return carry

        if active:
            lax.fori_loop(start, stop, body, 0)

    def finish(c, carry):
        copy(c).wait()
        return carry

    lax.fori_loop(0, early, finish, 0)


def outer_kernel(
    low_ref, high_ref, yb_in, yd_in, zd_in, yi_in, tail, _, out_ref,
    box, der, inv, yb, yd, zd, yi, obuf, sem,
):
    nx, ny = out_ref.shape[1], out_ref.shape[2]
    rows = ny + 8
    late = pltpu.make_async_copy(
        tail, out_ref.at[:, pl.ds(nx - 2 - tail.shape[1], tail.shape[1])], sem.at[4]
    )
    late.start()

    def finish(k):
        x = k if k < 2 else nx - 4 + k
        return pltpu.make_async_copy(
            obuf.at[:, pl.ds(k, 1)], out_ref.at[:, pl.ds(x, 1)], sem.at[k]
        )

    lane = lanes((rows, 128))
    for k, (ref, s) in enumerate(((low_ref, 0), (low_ref, 1), (high_ref, 0), (high_ref, 1))):
        v = ref[s * rows : (s + 1) * rows]
        packed = ref[2 * rows : 2 * rows + 8]
        h = jnp.concatenate(
            [pltpu.roll(packed, (126 - 8 * g - 4 * s) % 128, 1) for g in range(rows // 8)], axis=0
        )
        for dst, value in zip((box, der, inv), zsums(v, h, lane)):
            put(dst, k, value, ny)
    for k in range(4):
        for r in range(0, ny, 16):
            for ref, value in zip((yb, yd, zd, yi), ysums((box, der, inv), k, 16, r)):
                ref[k, r : r + 16] = value
    for side in range(2):
        for s in range(2):
            def pick(halo_ref, own_ref, j, part):
                x = s + j
                if side == 0:
                    return halo_ref[2 + x, part] if x < 0 else own_ref[x, part]
                x = x - 2
                return halo_ref[2 + x, part] if x >= 0 else own_ref[nx + x, part]

            for r in range(0, ny, 16):
                part = slice(r, r + 16)
                values = result(
                    [pick(yb, yb_in, j, part) for j in (-2, -1, 0, 1, 2)],
                    *[
                        [pick(h, o, j, part) for j in (-1, 0, 1)]
                        for h, o in ((yd, yd_in), (zd, zd_in), (yi, yi_in))
                    ],
                )
                for n, value in enumerate(values):
                    obuf[n, 2 * side + s, part] = value.astype(jnp.bfloat16)
            finish(2 * side + s).start()
    for k in range(4):
        finish(k).wait()
    late.wait()


def cost(us):
    return pl.CostEstimate(flops=int(us * 4e6), bytes_accessed=int(us * 1e6), transcendentals=0)


def shape(*dims, dtype=F32):
    return jax.ShapeDtypeStruct(dims, dtype)


def local(material, eps_table, grading):
    nx, ny, nz = material.shape
    rows = ny + 8
    material, eps_table, grading = (
        pltpu.with_memory_space_constraint(a, pltpu.HBM) for a in (material, eps_table, grading)
    )
    forward = [(i, (i + 1) % 8) for i in range(8)]
    backward = [(b, a) for a, b in forward]
    pairs = [[0, 1], [2, 3], [4, 5], [6, 7]]
    odd = [((i + 1) % 8, ((i ^ 1) + 1) % 8) for i in range(8)]
    parity = (lax.axis_index("gz") & 1).reshape(1)
    vmem = pltpu.CompilerParams(vmem_limit_bytes=24 << 20)

    y_face = shape(2 * nx + 8, nz)
    y_fwd, y_bwd, mat_near, gra_near, table_rows = pl.pallas_call(
        face_kernel,
        in_specs=[HBM] * 3,
        out_specs=[VMEM] * 5,
        out_shape=[
            y_face,
            y_face,
            shape(nx, ny, nz, dtype=jnp.int32),
            shape(nx, ny, nz, dtype=jnp.bfloat16),
            shape(8, nz),
        ],
        scratch_shapes=[
            pltpu.SMEM((8,), F32),
            pltpu.SemaphoreType.DMA((3, nx // STEP)),
        ],
        compiler_params=vmem,
        cost_estimate=cost(1),
        name="face",
    )(eps_table, material, grading)
    y_low = lax.ppermute(y_fwd, "gy", forward)
    y_high = lax.ppermute(y_bwd, "gy", backward)

    eps, packed = pl.pallas_call(
        block_kernel,
        in_specs=[VMEM] * 3,
        out_specs=[VMEM] * 2,
        out_shape=[shape(nx, ny, nz), shape(ny, nz)],
        compiler_params=vmem,
        cost_estimate=cost(3),
        name="block",
    )(table_rows, mat_near, gra_near)

    z_face = pl.pallas_call(
        zface_kernel,
        in_specs=[VMEM] * 3,
        out_specs=VMEM,
        out_shape=shape(rows, nz),
        compiler_params=vmem,
        cost_estimate=cost(0.2),
        name="zface",
    )(packed, y_low, y_high)
    z_odd = lax.ppermute(z_face, "gz", odd)
    z_even = lax.all_gather(z_face, "gz", axis=0, axis_index_groups=pairs)

    x_fwd, x_bwd = pl.pallas_call(
        xface_kernel,
        in_specs=[SMEM] + [VMEM] * 5,
        out_specs=[VMEM, VMEM],
        out_shape=[shape(2 * rows + 8, nz)] * 2,
        compiler_params=vmem,
        cost_estimate=cost(0.5),
        name="xface",
    )(parity, eps, y_low, y_high, z_even, z_odd)
    x_low = lax.ppermute(x_fwd, "gx", forward)
    x_high = lax.ppermute(x_bwd, "gx", backward)

    full = (nx, ny + 16, nz)
    late = nx - 4 - EARLY * GROUP
    out, *edges = pl.pallas_call(
        inner_kernel,
        in_specs=[SMEM] + [VMEM] * 5,
        out_specs=[ANY] + [VMEM] * 5,
        out_shape=[shape(6, nx, ny, nz, dtype=jnp.bfloat16)]
        + [shape(nx, ny, nz)] * 4
        + [shape(6, late, ny, nz, dtype=jnp.bfloat16)],
        scratch_shapes=[
            pltpu.VMEM((nx, 8, nz), F32),
            pltpu.VMEM((rows, nz), F32),
            pltpu.VMEM((nx, rows, nz), F32),
            pltpu.VMEM((512, 256), jnp.bfloat16),
            *[pltpu.VMEM((nx, ny + 16, nz), F32)] * 3,
            pltpu.VMEM((6, nx - 4 - late, ny, nz), jnp.bfloat16),
            pltpu.SemaphoreType.DMA(((nx - 4 - late) // GROUP,)),
        ],
        compiler_params=vmem,
        cost_estimate=cost(6),
        name="inner",
    )(parity, eps, y_low, y_high, z_even, z_odd)

    return pl.pallas_call(
        outer_kernel,
        in_specs=[VMEM] * 7 + [ANY],
        out_specs=ANY,
        out_shape=shape(6, nx, ny, nz, dtype=jnp.bfloat16),
        input_output_aliases={7: 0},
        scratch_shapes=[
            *[pltpu.VMEM((4, ny + 16, nz), F32)] * 3,
            *[pltpu.VMEM((4, ny, nz), F32)] * 4,
            pltpu.VMEM((6, 4, ny, nz), jnp.bfloat16),
            pltpu.SemaphoreType.DMA((5,)),
        ],
        compiler_params=vmem,
        cost_estimate=cost(1),
        name="outer",
    )(x_low, x_high, *edges, out)


def solution(mesh):
    return jax.shard_map(
        local,
        mesh=mesh,
        in_specs=(P("gx", "gy", "gz"), P(), P("gx", "gy", "gz")),
        out_specs=P(None, "gx", "gy", "gz"),
        check_vma=False,
    )
```
